32 devices in a mesh: sec: 2 (over x), tile: 16 (over z, y, core).
Axes of the slice: x: 2, y: 2, z: 4, core: 2. Of those that a mesh axis runs over, the one named last changes fastest.
Arguments:
- atmosphere: bfloat16 [32, 360, 384], P(('sec', 'tile')), may hold values from -6 to 6
- ocean_state: bfloat16 [128, 1440, 128], P('tile', 'sec'), may hold values from -6 to 6
- land_mask: int32 [128, 1440], P('tile', 'sec'), may hold values 0 or 1
- crossing_bands: int32 [16, 4], P('tile'), may hold values from 0 to 31, as said below
- ocean_regrid: float32 [16, 4, 8, 1], P('tile'), may hold values from 0 to 1, as said below
- atmosphere_regrid: float32 [16, 4, 1, 8], P('tile'), may hold values from 0 to 1, as said below
- surface_read: bfloat16 [128], replicated, may hold values from -0.5 to 0.5
- surface_embed: float32 [384], replicated, may hold values from -4 to 4
- flux_read: bfloat16 [384, 8], replicated, may hold values from -0.3125 to 0.3125
- flux_embed: bfloat16 [8, 128], replicated, may hold values from -2 to 2
- legendre_forward: bfloat16 [128, 32, 32], P(('sec', 'tile')), may hold values from -1 to 1
- legendre_inverse: bfloat16 [128, 32, 32], P(('sec', 'tile')), may hold values from -1 to 1
- spectral_mix: bfloat16 [2, 384, 384], replicated, may hold values from -0.3125 to 0.3125
- conv_kernel: bfloat16 [2, 7, 7, 128], replicated, may hold values from -0.875 to 0.875
- norm_gain: float32 [2, 128], replicated, may hold values from 0.1 to 1.9
- expand_weight: bfloat16 [2, 128, 512], replicated, may hold values from -0.5 to 0.5
- project_weight: bfloat16 [2, 512, 128], replicated, may hold values from -0.25 to 0.25
- atmosphere_cotangent: bfloat16 [32, 360, 384], P(('sec', 'tile')), may hold values from -6 to 6
- ocean_cotangent: bfloat16 [128, 1440, 128], P('tile', 'sec'), may hold values from -6 to 6
Outputs:
- atmosphere_next: bfloat16 [32, 360, 384], P(('sec', 'tile'))
- ocean_next: bfloat16 [128, 1440, 128], P('tile', 'sec')
- atmosphere_grad: float32 [32, 360, 384], P(('sec', 'tile'))
- ocean_grad: float32 [128, 1440, 128], P('tile', 'sec')
The draws below stay inside these ranges and needn't reach their ends.
Inputs may be any that keep to these rules, and one draw needn't show every extreme that they name: `crossing_bands`: row j lists between 1 and 4 consecutive distinct atmosphere bands, then repeats its last band; some row lists 4. Its first band is j * 2 - 1, j * 2 or j * 2 + 1, raised to 0 or lowered as far as needed for the list to end at band 32 - 1 at most. `ocean_regrid`: zero in the repeated slots of crossing_bands; the entries of each ocean row sum to one. `atmosphere_regrid`: zero in the repeated slots of crossing_bands.
All inputs are finite; a program needn't handle non-finite values. No bound on the sum of `land_mask` on one device may be relied on, other than what follows from the above.
Results may differ from the reference program's by a relative error of at most 0.008.
Values may be sent and summed in bfloat16 or wider, within the bound.
A program may use at most 128 MiB of HBM per device.

```python
import jax
import jax.numpy as jnp
from jax import lax

C = 384
ALON = 360
MODES = 128
F = 8
OC = 128
OHID = 512
KS = 7
LAYERS = 2
PEERS = 4
ALAT_DEV = 1
OLAT_DEV = 8
BANDS = 32
GROUPS = 16
ALAT = 32
OLAT = 128
OLON = 1440


def crossing_layout(key):
    base = jax.random.fold_in(key, 17)
    count_key, step_key = jax.random.split(base)
    group_index = jnp.arange(GROUPS, dtype=jnp.int32)
    counts = jax.random.randint(count_key, (GROUPS,), 1, PEERS + 1).astype(jnp.int32)
    counts = jnp.where(group_index == GROUPS // 2, PEERS, counts)
    wiggle = jax.random.randint(step_key, (GROUPS,), -1, 2).astype(jnp.int32)
    first = group_index * (BANDS // GROUPS) + wiggle
    first = jnp.minimum(jnp.maximum(first, 0), BANDS - counts)
    slot = jnp.arange(PEERS, dtype=jnp.int32)
    listed = first[:, None] + jnp.minimum(slot[None, :], counts[:, None] - 1)
    valid = (slot[None, :] < counts[:, None]).astype(jnp.float32)
    return (listed.astype(jnp.int32), valid)


def positive_weights(key, shape):
    raw = jax.random.uniform(key, shape, jnp.float32, 0.2, 1.0)
    return raw


def draw_crossing_bands(key, part):
    return crossing_layout(key)[0]


def draw_ocean_regrid(key, part):
    listed, valid = crossing_layout(key)
    raw = positive_weights(jax.random.fold_in(key, 29), (GROUPS, PEERS, OLAT_DEV, ALAT_DEV))
    raw = raw * valid[:, :, None, None]
    return raw / jnp.sum(raw, axis=(1, 3), keepdims=True)


def draw_atmosphere_regrid(key, part):
    listed, valid = crossing_layout(key)
    raw = positive_weights(jax.random.fold_in(key, 31), (GROUPS, PEERS, ALAT_DEV, OLAT_DEV))
    return raw * valid[:, :, None, None] / OLAT_DEV


def touch_ends(array, own_key, smallest, largest):
    place = [jax.random.randint(jax.random.fold_in(own_key, axis), (), 0, length) for axis, length in enumerate(array.shape)]
    widest = array.shape.index(max(array.shape))
    beside = place[:widest] + [(place[widest] + 1) % array.shape[widest]] + place[widest + 1:]
    return array.at[tuple(place)].set(smallest).at[tuple(beside)].set(largest)


def shard_levels(rng, shape, cuts, least, high):
    def one(axis_at, shards_of):
        steps = jax.random.uniform(jax.random.fold_in(jax.random.fold_in(rng, 6), axis_at), (shards_of,), jnp.float32, least / len(cuts), high / len(cuts))
        return jnp.repeat(jnp.exp(steps), shape[axis_at] // shards_of).reshape((-1,) + (1,) * (len(shape) - axis_at - 1))

    loudness = one(*cuts[0])
    for cut in cuts[1:]:
        loudness = loudness * one(*cut)
    return loudness


def centred(stream_key, shape, deviation, limit, cuts=(), kind=jnp.bfloat16):
    entries = jax.random.normal(stream_key, shape, jnp.float32) * deviation
    if len(cuts) > 0:
        entries = shard_levels(stream_key, shape, cuts, -0.22, 0.18) * entries
    return jnp.clip(entries, min=-limit, max=limit).astype(kind)


def setup_inputs(seed: int = 0) -> dict:
    arg_keys = jax.random.split(jax.random.key(seed), 20)
    return {
        "atmosphere": centred(arg_keys[0], (ALAT, ALON, C), 1.0, 6.0, ((0, 32),)),
        "ocean_state": centred(arg_keys[1], (OLAT, OLON, OC), 1.0, 6.0, ((0, 16), (1, 2))),
        "land_mask": touch_ends((jax.random.randint(arg_keys[2], (OLAT, OLON), 0, 10) < 7).astype(jnp.int32), jax.random.fold_in(arg_keys[2], 1), 0, 1),
        "crossing_bands": draw_crossing_bands(jax.random.fold_in(arg_keys[19], 71), 0),
        "ocean_regrid": draw_ocean_regrid(jax.random.fold_in(arg_keys[19], 71), 0),
        "atmosphere_regrid": draw_atmosphere_regrid(jax.random.fold_in(arg_keys[19], 71), 0),
        "surface_read": centred(arg_keys[6], (OC,), OC ** -0.5, 0.5),
        "surface_embed": centred(arg_keys[7], (C,), 1.0, 4.0, (), jnp.float32),
        "flux_read": centred(arg_keys[8], (C, F), C ** -0.5, 0.3125),
        "flux_embed": centred(arg_keys[9], (F, OC), F ** -0.5, 2.0),
        "legendre_forward": centred(arg_keys[10], (MODES, ALAT, ALAT), ALAT ** -0.5, 1.0, ((0, 32),)),
        "legendre_inverse": centred(arg_keys[11], (MODES, ALAT, ALAT), ALAT ** -0.5, 1.0, ((0, 32),)),
        "spectral_mix": centred(arg_keys[12], (2, C, C), C ** -0.5, 0.3125),
        "conv_kernel": centred(arg_keys[13], (LAYERS, KS, KS, OC), (KS * KS) ** -0.5, 0.875),
        "norm_gain": jnp.clip(1.0 + 0.18 * jax.random.normal(arg_keys[14], (LAYERS, OC), jnp.float32), 0.1, 1.9),
        "expand_weight": centred(arg_keys[15], (LAYERS, OC, OHID), OC ** -0.5, 0.5),
        "project_weight": centred(arg_keys[16], (LAYERS, OHID, OC), OHID ** -0.5, 0.25),
        "atmosphere_cotangent": centred(arg_keys[17], (ALAT, ALON, C), 1.0, 6.0, ((0, 32),)),
        "ocean_cotangent": centred(arg_keys[18], (OLAT, OLON, OC), 1.0, 6.0, ((0, 16), (1, 2))),
    }


def wave_table(lon_count, mode_count):
    longitude = jnp.arange(lon_count, dtype=jnp.int32)
    wavenumber = jnp.arange(mode_count, dtype=jnp.int32)
    phase = (longitude[:, None] * wavenumber[None, :] % lon_count).astype(jnp.float32) * (2.0 * jnp.pi / lon_count)
    scaled = jnp.stack([jnp.cos(phase), -jnp.sin(phase)], axis=2) * jnp.sqrt(jnp.float32(2.0 / lon_count))
    return scaled.reshape(lon_count, 2 * mode_count).astype(jnp.bfloat16)

def depthwise(window, kernel):
    radius = kernel.shape[0] // 2
    height = window.shape[0] - 2 * radius
    extent = window.shape[1]
    wide = jnp.concatenate([window[:, extent - radius:], window, window[:, :radius]], axis=1).astype(jnp.float32)
    weights = kernel.astype(jnp.float32)
    total = jnp.zeros((height, extent, window.shape[2]), jnp.float32)
    for shift_row in range(kernel.shape[0]):
        for shift_col in range(kernel.shape[1]):
            total = total + wide[shift_row:shift_row + height, shift_col:shift_col + extent] * weights[shift_row, shift_col]
    return total

def cell_forward(hidden, gain, expand, project):
    center = hidden - lax.optimization_barrier(jnp.mean(hidden, axis=-1, keepdims=True))
    inverse_std = lax.rsqrt(lax.optimization_barrier(jnp.mean(center * center, axis=-1, keepdims=True)) + 1e-06)
    normed = (center * inverse_std * gain).astype(jnp.bfloat16)
    before = jnp.dot(normed, expand, preferred_element_type=jnp.float32)
    active = jax.nn.gelu(before).astype(jnp.bfloat16)
    return jnp.dot(active, project, preferred_element_type=jnp.float32)

def cell_backward(hidden, gain, expand, project, mask_value, cotangent):
    center = hidden - lax.optimization_barrier(jnp.mean(hidden, axis=-1, keepdims=True))
    inverse_std = lax.rsqrt(lax.optimization_barrier(jnp.mean(center * center, axis=-1, keepdims=True)) + 1e-06)
    unit = center * inverse_std
    normed = (unit * gain).astype(jnp.bfloat16)
    before = jnp.dot(normed, expand, preferred_element_type=jnp.float32)
    masked = (mask_value[:, :, None] * cotangent).astype(jnp.bfloat16)
    active_adjoint = jnp.dot(masked, project.T, preferred_element_type=jnp.float32)
    _, gelu_back = jax.vjp(jax.nn.gelu, before)
    before_adjoint = gelu_back(active_adjoint)[0].astype(jnp.bfloat16)
    normed_adjoint = jnp.dot(before_adjoint, expand.T, preferred_element_type=jnp.float32)
    scaled = normed_adjoint * gain
    result = inverse_std * (scaled - lax.optimization_barrier(jnp.mean(scaled, axis=-1, keepdims=True)) - unit * lax.optimization_barrier(jnp.mean(scaled * unit, axis=-1, keepdims=True)))
    return result.astype(jnp.bfloat16)

def ocean_matrix(bands_row, blocks, lat_count):
    lat_band = blocks.shape[2]
    index = bands_row[:, None] * lat_band + jnp.arange(lat_band, dtype=jnp.int32)[None, :]
    onehot = (index[:, :, None] == jnp.arange(lat_count, dtype=jnp.int32)[None, None, :]).astype(jnp.float32)
    return jnp.einsum('poi,pia->oa', blocks, onehot, precision=lax.Precision.HIGHEST)

def atmosphere_matrix(bands_row, blocks, lat_count):
    lat_band = blocks.shape[1]
    index = bands_row[:, None] * lat_band + jnp.arange(lat_band, dtype=jnp.int32)[None, :]
    onehot = (index[:, :, None] == jnp.arange(lat_count, dtype=jnp.int32)[None, None, :]).astype(jnp.float32)
    return jnp.einsum('pio,pia->ao', blocks, onehot, precision=lax.Precision.HIGHEST)

def mix_complex(coefficient, mix_real, mix_imag):
    real_part = coefficient[:, :, 0].astype(jnp.float32)
    imag_part = coefficient[:, :, 1].astype(jnp.float32)
    first = mix_real.astype(jnp.float32)
    second = mix_imag.astype(jnp.float32)
    out_real = jnp.einsum('lmc,cd->lmd', real_part, first) - jnp.einsum('lmc,cd->lmd', imag_part, second)
    out_imag = jnp.einsum('lmc,cd->lmd', imag_part, first) + jnp.einsum('lmc,cd->lmd', real_part, second)
    return jnp.stack([out_real, out_imag], axis=2).astype(jnp.bfloat16)

def spectral_block(spectrum, forward, inverse, mixing):
    lat_count, columns, channels = spectrum.shape
    split = spectrum.reshape(lat_count, columns // 2, 2, channels).astype(jnp.float32)
    coefficient = jnp.einsum('mla,amrc->lmrc', forward.astype(jnp.float32), split).astype(jnp.bfloat16)
    mixed = mix_complex(coefficient, mixing[0], mixing[1])
    returned = jnp.einsum('mal,lmrc->amrc', inverse.astype(jnp.float32), mixed.astype(jnp.float32)).astype(jnp.bfloat16)
    return returned.reshape(lat_count, columns, channels)

def spectral_adjoint(returned_adjoint, forward, inverse, mixing):
    lat_count, columns, channels = returned_adjoint.shape
    split = returned_adjoint.reshape(lat_count, columns // 2, 2, channels).astype(jnp.float32)
    mixed_adjoint = jnp.einsum('mal,amrc->lmrc', inverse.astype(jnp.float32), split).astype(jnp.bfloat16)
    real_part = mixed_adjoint[:, :, 0].astype(jnp.float32)
    imag_part = mixed_adjoint[:, :, 1].astype(jnp.float32)
    first = mixing[0].astype(jnp.float32)
    second = mixing[1].astype(jnp.float32)
    back_real = jnp.einsum('lmd,cd->lmc', real_part, first) + jnp.einsum('lmd,cd->lmc', imag_part, second)
    back_imag = jnp.einsum('lmd,cd->lmc', imag_part, first) - jnp.einsum('lmd,cd->lmc', real_part, second)
    coefficient_adjoint = jnp.stack([back_real, back_imag], axis=2).astype(jnp.bfloat16)
    spectrum_adjoint = jnp.einsum('mla,lmrc->amrc', forward.astype(jnp.float32), coefficient_adjoint.astype(jnp.float32)).astype(jnp.bfloat16)
    return spectrum_adjoint.reshape(lat_count, columns, channels)

def ocean_layer(state, mask_value, kernel, gain, expand, project, band):
    radius = kernel.shape[0] // 2
    padded = jnp.pad(state, ((radius, radius), (0, 0), (0, 0)))
    band_count = state.shape[0] // band

    def one_band(index):
        start = index * band
        window = lax.dynamic_slice_in_dim(padded, start, band + 2 * radius, 0)
        update = cell_forward(depthwise(window, kernel), gain, expand, project)
        own = lax.dynamic_slice_in_dim(state, start, band, 0).astype(jnp.float32)
        weight = lax.dynamic_slice_in_dim(mask_value, start, band, 0)
        return (own + weight[:, :, None] * update).astype(jnp.bfloat16)
    result = lax.map(one_band, jnp.arange(band_count, dtype=jnp.int32))
    return result.reshape(state.shape)

def ocean_layer_adjoint(state, mask_value, kernel, gain, expand, project, cotangent, band):
    radius = kernel.shape[0] // 2
    padded = jnp.pad(state, ((radius, radius), (0, 0), (0, 0)))
    band_count = state.shape[0] // band

    def local_adjoint(index):
        start = index * band
        window = lax.dynamic_slice_in_dim(padded, start, band + 2 * radius, 0)
        hidden = depthwise(window, kernel)
        local_cotangent = lax.dynamic_slice_in_dim(cotangent, start, band, 0)
        weight = lax.dynamic_slice_in_dim(mask_value, start, band, 0)
        return cell_backward(hidden, gain, expand, project, weight, local_cotangent)
    hidden_adjoint = lax.map(local_adjoint, jnp.arange(band_count, dtype=jnp.int32)).reshape(state.shape)
    padded_adjoint = jnp.pad(hidden_adjoint, ((radius, radius), (0, 0), (0, 0)))
    flipped = kernel[::-1, ::-1]

    def spread(index):
        start = index * band
        window = lax.dynamic_slice_in_dim(padded_adjoint, start, band + 2 * radius, 0)
        return depthwise(window, flipped)
    spreads = lax.map(spread, jnp.arange(band_count, dtype=jnp.int32)).reshape(state.shape)
    return cotangent + spreads

def reference(atmosphere, ocean_state, land_mask, crossing_bands, ocean_regrid, atmosphere_regrid, surface_read, surface_embed, flux_read, flux_embed, legendre_forward, legendre_inverse, spectral_mix, conv_kernel, norm_gain, expand_weight, project_weight, atmosphere_cotangent, ocean_cotangent):
    group_total = crossing_bands.shape[0]
    lat_count, lon_count, channels = atmosphere.shape
    ocean_rows, ocean_lon, ocean_channels = ocean_state.shape
    band = ocean_rows // group_total
    ratio = ocean_lon // lon_count
    flux_count = flux_read.shape[1]
    highest = lax.Precision.HIGHEST
    to_ocean = jax.vmap(lambda row, blocks: ocean_matrix(row, blocks, lat_count))(crossing_bands, ocean_regrid)
    to_ocean = to_ocean.reshape(ocean_rows, lat_count)
    to_atmosphere = jax.vmap(lambda row, blocks: atmosphere_matrix(row, blocks, lat_count))(crossing_bands, atmosphere_regrid)
    to_atmosphere = jnp.transpose(to_atmosphere, (1, 0, 2)).reshape(lat_count, ocean_rows)
    mask_value = land_mask.astype(jnp.float32)
    surface = jnp.dot(ocean_state, surface_read, preferred_element_type=jnp.float32)
    coarse = lax.optimization_barrier(jnp.mean((mask_value * surface).reshape(ocean_rows, lon_count, ratio), axis=2))
    surface_atmosphere = jnp.dot(to_atmosphere, coarse, precision=highest)
    mixed_input = (atmosphere.astype(jnp.float32) + surface_atmosphere[:, :, None] * surface_embed[None, None, :]).astype(jnp.bfloat16)
    table = wave_table(lon_count, legendre_forward.shape[0]).astype(jnp.float32)
    spectrum = jnp.einsum('gk,agc->akc', table, mixed_input.astype(jnp.float32)).astype(jnp.bfloat16)
    returned = spectral_block(spectrum, legendre_forward, legendre_inverse, spectral_mix)
    response = jnp.einsum('gk,akc->agc', table, returned.astype(jnp.float32))
    atmosphere_next = (mixed_input.astype(jnp.float32) + jax.nn.gelu(response)).astype(jnp.bfloat16)
    flux = jnp.einsum('agc,cf->agf', atmosphere.astype(jnp.float32), flux_read.astype(jnp.float32))
    flux_ocean = jnp.dot(to_ocean, flux.reshape(lat_count, lon_count * flux_count), precision=highest)
    forcing_coarse = jnp.einsum('ogf,fc->ogc', flux_ocean.reshape(ocean_rows, lon_count, flux_count), flux_embed.astype(jnp.float32), precision=highest)
    forcing = jnp.broadcast_to(forcing_coarse[:, :, None, :], (ocean_rows, lon_count, ratio, ocean_channels)).reshape(ocean_rows, ocean_lon, ocean_channels)
    state = (ocean_state.astype(jnp.float32) + mask_value[:, :, None] * forcing).astype(jnp.bfloat16)
    states = []
    for layer in range(conv_kernel.shape[0]):
        states.append(state)
        state = ocean_layer(state, mask_value, conv_kernel[layer], norm_gain[layer], expand_weight[layer], project_weight[layer], band)
    ocean_next = state
    cotangent = ocean_cotangent.astype(jnp.float32)
    for layer in range(conv_kernel.shape[0] - 1, -1, -1):
        cotangent = ocean_layer_adjoint(states[layer], mask_value, conv_kernel[layer], norm_gain[layer], expand_weight[layer], project_weight[layer], cotangent, band)
    forcing_adjoint = (mask_value[:, :, None] * cotangent).reshape(ocean_rows, lon_count, ratio, ocean_channels).sum(axis=2)
    flux_ocean_adjoint = jnp.einsum('ogc,fc->ogf', forcing_adjoint, flux_embed.astype(jnp.float32), precision=highest)
    flux_adjoint = jnp.dot(to_ocean.T, flux_ocean_adjoint.reshape(ocean_rows, lon_count * flux_count), precision=highest)
    flux_adjoint = flux_adjoint.reshape(lat_count, lon_count, flux_count)
    from_flux = jnp.einsum('agf,cf->agc', flux_adjoint, flux_read.astype(jnp.float32), precision=highest)
    atmosphere_adjoint = atmosphere_cotangent.astype(jnp.float32)
    _, gelu_back = jax.vjp(jax.nn.gelu, response)
    response_adjoint = gelu_back(atmosphere_adjoint)[0].astype(jnp.bfloat16)
    returned_adjoint = jnp.einsum('gk,agc->akc', table, response_adjoint.astype(jnp.float32)).astype(jnp.bfloat16)
    spectrum_adjoint = spectral_adjoint(returned_adjoint, legendre_forward, legendre_inverse, spectral_mix)
    input_adjoint = atmosphere_adjoint + jnp.einsum('gk,akc->agc', table, spectrum_adjoint.astype(jnp.float32))
    atmosphere_grad = input_adjoint + from_flux
    surface_adjoint = jnp.einsum('agc,c->ag', input_adjoint, surface_embed, precision=highest)
    coarse_adjoint = jnp.dot(to_atmosphere.T, surface_adjoint, precision=highest)
    widened = jnp.broadcast_to(coarse_adjoint[:, :, None], (ocean_rows, lon_count, ratio)).reshape(ocean_rows, ocean_lon)
    surface_grad = mask_value * widened / ratio
    ocean_grad = cotangent + surface_grad[:, :, None] * surface_read.astype(jnp.float32)[None, None, :]
    return (atmosphere_next, ocean_next, atmosphere_grad, ocean_grad)
```

```python
import functools

import jax
import jax.numpy as jnp
import numpy as np
from jax import lax
from jax.experimental import pallas as pl
from jax.experimental.pallas import tpu as pltpu
from jax.sharding import PartitionSpec as P

MESH = pl.DeviceIdType.MESH
F32 = jnp.float32
BF16 = jnp.bfloat16
GELU_SCALE = 0.7978845608028654
GELU_CUBIC = 0.044715
EPSILON = 1e-06
MARGIN = 16
SLOTS = 8
LANES = 128


def wave_table(lon_count, mode_count):
    longitude = np.arange(lon_count)
    wavenumber = np.arange(mode_count)
    phase = (longitude[:, None] * wavenumber[None, :] % lon_count) * (2.0 * np.pi / lon_count)
    scaled = np.stack([np.cos(phase), -np.sin(phase)], axis=2) * np.sqrt(2.0 / lon_count)
    return scaled.reshape(lon_count, 2 * mode_count).astype(np.float32).astype(BF16)


def mode_order(lat_count, modes):
    source = np.arange(lat_count * modes * 2)
    lat, mode, part = source // (2 * modes), source % (2 * modes) // 2, source % 2
    matrix = np.zeros((source.size, source.size), np.float32)
    matrix[(part * modes + mode) * lat_count + lat, source] = 1.0
    return matrix.astype(BF16)


def dot(a, b):
    return lax.dot_general(a, b, (((1,), (0,)), ((), ())), preferred_element_type=F32)


def dot_nt(a, b):
    return lax.dot_general(a, b, (((1,), (1,)), ((), ())), preferred_element_type=F32)


def dot_tn(a, b):
    return lax.dot_general(a, b, (((0,), (0,)), ((), ())), preferred_element_type=F32)


def halves(x):
    high = x.astype(BF16)
    return high, (x - high.astype(F32)).astype(BF16)


def loop(count, body):
    def step(index, carry):
        body(index)
        return carry

    lax.fori_loop(0, count, step, jnp.int32(0))


def normalize(hidden):
    center = hidden - jnp.mean(hidden, axis=-1, keepdims=True)
    inverse_std = lax.rsqrt(jnp.mean(center * center, axis=-1, keepdims=True) + EPSILON)
    return center * inverse_std, inverse_std


def gelu_parts(before):
    square = before * before
    wave = jnp.tanh(before * (GELU_SCALE + (GELU_SCALE * GELU_CUBIC) * square))
    return square, wave


def gelu_value(before, wave):
    scaled = 0.5 * before
    return scaled + scaled * wave


def gelu_slope(before, square, wave):
    slope = (0.5 * GELU_SCALE + (1.5 * GELU_SCALE * GELU_CUBIC) * square) * before
    return 0.5 + 0.5 * wave + slope * (1.0 - wave * wave)


def window_kernel(
    axes,
    atm, ocean, mask, bands, oreg, areg, read, embed, flux_read_t, flux_embed,
    leg_f, leg_i, smix, taps_in, gains, expand, project, acot, ocot,
    table, table_t, order, order_t,
    atm_next, ocean_next, atm_grad, ocean_grad,
    win, wide, hid, taps, mask_wide, repeat, surf, gall, fold,
    wo, wa, flux_send, flux_recv, cp_send, cp_recv, sa_send, sa_recv, fa_send, fa_recv,
    xs, xr, flat, mixed, spec_a, spec_b,
    halo_send, halo_recv, x_send, x_recv, near_send, near_recv,
):
    sections, tiles = axes
    devices = sections * tiles
    sec = lax.axis_index("sec")
    tile = lax.axis_index("tile")
    me = sec * tiles + tile
    rows, extent, channels = ocean.shape
    lon = atm.shape[0]
    radius = (win.shape[1] - rows) // 2
    side = 2 * radius + 1
    part = lon // sections
    ratio = extent // part
    cols = xs.shape[2]
    right = MARGIN + extent

    def target(device):
        return {"sec": lax.div(device, tiles), "tile": lax.rem(device, tiles)}

    barrier = pltpu.get_barrier_semaphore()

    def greet(step):
        pl.semaphore_signal(
            barrier, inc=1, device_id=target(lax.rem(me + 1 + step, devices)), device_id_type=MESH
        )

    loop(devices - 1, greet)

    @pl.when(tile == 0)
    def _():
        win[:, 0:radius] = jnp.zeros((win.shape[0], radius) + win.shape[2:], BF16)

    @pl.when(tile == tiles - 1)
    def _():
        win[:, radius + rows :] = jnp.zeros((win.shape[0], radius) + win.shape[2:], BF16)

    x_index = lax.broadcasted_iota(jnp.int32, (extent, lon), 0)
    g_index = lax.broadcasted_iota(jnp.int32, (extent, lon), 1)
    offset = x_index - (g_index - sec * part) * ratio
    repeat[...] = jnp.where((offset >= 0) & (offset < ratio), 1.0, 0.0).astype(BF16)

    for row in range(rows):
        surf[row : row + 1, :] = dot_nt(read[...], ocean[row])
    mask_value = mask[...].astype(F32)
    high, low = halves(surf[...] * mask_value * (1.0 / ratio))
    surf[:, 0:lon] = dot(high, repeat[...]) + dot(low, repeat[...])

    flux_send[...] = dot_nt(flux_read_t[...], atm[...])

    def weights(slot):
        band = lax.rem(2 * tile - 2 + slot + devices, devices)
        for row in range(rows):
            to_ocean = jnp.float32(0.0)
            to_atm = jnp.float32(0.0)
            for peer in range(bands.shape[1]):
                same = jnp.where(bands[0, peer] == band, 1.0, 0.0)
                to_ocean = to_ocean + same * oreg[peer, row]
                to_atm = to_atm + same * areg[peer, row]
            wo[slot, row] = to_ocean
            wa[slot, row] = to_atm

    loop(SLOTS, weights)

    def coarse_part(slot):
        total = wa[slot, 0] * surf[0:1, 0:lon]
        for row in range(1, rows):
            total = total + wa[slot, row] * surf[row : row + 1, 0:lon]
        cp_send[slot] = total

    loop(SLOTS, coarse_part)

    pl.semaphore_wait(barrier, devices - 1)

    def band_to_groups(index, source, slots, act):
        def one(step):
            turn, section = lax.div(step, sections), lax.rem(step, sections)
            group = lax.rem(lax.div(me, 2) + 1 - turn + tiles, tiles)
            slot = lax.rem(me, 2) + 2 * turn
            away = (section != sec) | (group != tile)

            def remote():
                return pltpu.make_async_remote_copy(
                    src_ref=source,
                    dst_ref=slots.at[slot],
                    send_sem=near_send.at[index, step],
                    recv_sem=near_recv.at[index],
                    device_id={"sec": section, "tile": group},
                    device_id_type=MESH,
                )

            @pl.when(away)
            def _():
                act(remote())

            if act is start:

                @pl.when(jnp.logical_not(away))
                def _():
                    pltpu.make_async_copy(source, slots.at[slot], near_recv.at[index]).start()

        loop(SLOTS // 2 * sections, one)

    def group_to_bands(index, parts, slots, act):
        def one(slot):
            band = lax.rem(2 * tile - 2 + slot + devices, devices)
            place = lax.div(slot, 2) * sections + sec

            def remote():
                return pltpu.make_async_remote_copy(
                    src_ref=parts.at[slot],
                    dst_ref=slots.at[place],
                    send_sem=near_send.at[index, slot],
                    recv_sem=near_recv.at[index],
                    device_id=target(band),
                    device_id_type=MESH,
                )

            @pl.when(band != me)
            def _():
                act(remote())

            if act is start:

                @pl.when(band == me)
                def _():
                    pltpu.make_async_copy(
                        parts.at[slot], slots.at[place], near_recv.at[index]
                    ).start()

        loop(SLOTS, one)

    def start(copy):
        copy.start()

    def sent(copy):
        copy.wait_send()

    def near_wait(index, slots):
        pltpu.make_async_copy(slots, slots, near_recv.at[index]).wait()

    def all_start(index):
        pltpu.make_async_copy(xs.at[index, me], xr.at[index, me], x_recv.at[index]).start()

        def one(step):
            peer = lax.rem(me + 1 + step, devices)
            pltpu.make_async_remote_copy(
                src_ref=xs.at[index, peer],
                dst_ref=xr.at[index, me],
                send_sem=x_send.at[index],
                recv_sem=x_recv.at[index],
                device_id=target(peer),
                device_id_type=MESH,
            ).start()

        loop(devices - 1, one)

    def all_wait(index):
        pltpu.make_async_copy(xr.at[index], xr.at[index], x_recv.at[index]).wait()

    def all_sent(index):
        others = xs.at[index, pl.ds(0, devices - 1)]
        pltpu.make_async_copy(others, others, x_send.at[index]).wait()

    def rim(layer, row_step, col_step):
        number = (row_step + 1) * 3 + col_step + 1
        number = number if number < 4 else number - 1
        source_rows = {-1: (radius, radius), 0: (radius, rows), 1: (rows, radius)}[row_step]
        place_rows = {-1: (radius + rows, radius), 0: (radius, rows), 1: (0, radius)}[row_step]
        inner = {-1: (MARGIN, MARGIN), 0: (MARGIN, extent), 1: (extent, MARGIN)}[col_step]
        outer = {-1: (right, MARGIN), 0: (MARGIN, extent), 1: (0, MARGIN)}[col_step]
        return pltpu.make_async_remote_copy(
            src_ref=win.at[layer, pl.ds(*source_rows), pl.ds(*inner)],
            dst_ref=win.at[layer, pl.ds(*place_rows), pl.ds(*outer)],
            send_sem=halo_send.at[layer, number],
            recv_sem=halo_recv.at[layer, number],
            device_id={
                "sec": lax.rem(sec + col_step + sections, sections),
                "tile": lax.rem(tile + row_step + tiles, tiles),
            },
            device_id_type=MESH,
        )

    def rims(layer, act, sending, row_steps):
        for row_step in row_steps:
            edge = {-1: 0, 0: None, 1: tiles - 1}[row_step if sending else -row_step]

            def each(row_step=row_step):
                for col_step in (0, -1, 1):
                    if (row_step, col_step) != (0, 0):
                        act(rim(layer, row_step, col_step))

            if edge is None:
                each()
            else:
                pl.when(tile != edge)(each)

    def rims_start(layer):
        rims(layer, lambda copy: copy.start(), True, (0, -1, 1))

    def rims_sent(layer):
        rims(layer, lambda copy: copy.wait_send(), True, (0, -1, 1))

    def rims_wait(layer, row_steps):
        rims(layer, lambda copy: copy.wait_recv(), False, row_steps)

    def widen(layer, first, count):
        def one(index):
            wide[first + index] = win[layer, first + index].astype(F32)

        loop(count, one)

    def depthwise(kernel, flip, lines, base, store):
        def step(index):
            begin = pl.multiple_of(index * 8, 8)
            totals = [None] * rows
            for col in range(side):
                tap = [
                    taps[kernel, side * side - 1 - (u * side + col) if flip else u * side + col]
                    for u in range(side)
                ]
                for line in lines:
                    piece = wide[line, pl.ds(begin + (MARGIN - radius + col), 8), :]
                    for u in range(side):
                        place = line - u
                        if 0 <= place < rows:
                            term = piece * tap[u]
                            old = totals[place]
                            totals[place] = term if old is None else old + term
            for row in range(rows):
                if totals[row] is not None:
                    before = base(row, begin)
                    store(row, begin, totals[row] if before is None else before + totals[row])

        loop(extent // 8, step)

    own_lines = range(radius, radius + rows)
    rim_lines = list(range(radius)) + list(range(radius + rows, rows + 2 * radius))

    def first_part(layer, kernel, flip, base, store):
        rims_wait(layer, (0,))
        widen(layer, radius, rows)
        depthwise(kernel, flip, own_lines, base, store)

    def second_part(layer, kernel, flip, base, store):
        rims_wait(layer, (-1, 1))
        widen(layer, 0, radius)
        widen(layer, radius + rows, radius)
        depthwise(kernel, flip, rim_lines, base, store)

    height = max(cols, 8)
    group = height // cols

    def unpack(index):
        def one(block):
            pieces = [
                xr[index, block * group + place].astype(F32) for place in range(group)
            ]
            flat[pl.ds(pl.multiple_of(block * height, height), height), :] = (
                pieces[0] if group == 1 else jnp.concatenate(pieces, axis=0)
            )

        loop(devices // group, one)
        return flat[...].astype(BF16)

    def pack(index, value):
        flat[...] = value

        def one(block):
            piece = flat[pl.ds(pl.multiple_of(block * height, height), height), :].astype(BF16)
            for place in range(group):
                xs[index, block * group + place] = piece[place * cols : (place + 1) * cols]

        loop(devices // group, one)
        all_start(index)

    def spectral(index, first, first_dot, second, second_dot, adjoint):
        modes, lat = first.shape[0], first.shape[1]
        half = modes * lat
        all_wait(index)
        spec_a[...] = dot(order[...], unpack(index)).astype(BF16)
        for block in range(2 * modes):
            piece = pl.ds(block * lat, lat)
            spec_b[piece] = first_dot(first[block % modes], spec_a[piece]).astype(BF16)
        real, imag = spec_b[0:half], spec_b[half : 2 * half]
        if adjoint:
            spec_a[0:half] = (dot_nt(real, smix[0]) + dot_nt(imag, smix[1])).astype(BF16)
            spec_a[half : 2 * half] = (dot_nt(imag, smix[0]) - dot_nt(real, smix[1])).astype(BF16)
        else:
            spec_a[0:half] = (dot(real, smix[0]) - dot(imag, smix[1])).astype(BF16)
            spec_a[half : 2 * half] = (dot(imag, smix[0]) + dot(real, smix[1])).astype(BF16)
        for block in range(2 * modes):
            piece = pl.ds(block * lat, lat)
            spec_b[piece] = second_dot(second[block % modes], spec_a[piece]).astype(BF16)
        pack(index + 1, dot(order_t[...], spec_b[...]))

    band_to_groups(0, flux_send, flux_recv, start)
    group_to_bands(1, cp_send, cp_recv, start)

    lane_row = lax.broadcasted_iota(jnp.int32, (rows, rows * LANES), 1)
    sub_row = lax.broadcasted_iota(jnp.int32, (rows, rows * LANES), 0)
    inside = (lane_row >= sub_row * LANES) & (lane_row < (sub_row + 1) * LANES)
    spread = jnp.where(inside, 1.0, 0.0).astype(BF16)
    column = dot_tn(mask_value.astype(BF16), spread)
    for row in range(rows):
        mask_wide[row] = column[:, row * LANES : (row + 1) * LANES].astype(BF16)

    def tap_tile(index):
        for kernel in range(taps.shape[0]):
            taps[kernel, index] = jnp.broadcast_to(
                taps_in[kernel, pl.ds(index, 1), :], (8, channels)
            )

    loop(side * side, tap_tile)

    near_wait(0, flux_recv)
    for row in range(rows):
        total = wo[0, row] * flux_recv[0]
        for slot in range(1, SLOTS):
            total = total + wo[slot, row] * flux_recv[slot]
        high, low = halves(total)
        embed_rows = flux_embed[...]
        gall[row] = (dot_tn(high, embed_rows) + dot_tn(low, embed_rows)).astype(BF16)

    def force(row):
        forcing = dot(repeat[...], gall[row])
        state = ocean[row].astype(F32) + mask_wide[row].astype(F32) * forcing
        win[0, row + radius, MARGIN:right, :] = state.astype(BF16)

    loop(rows, force)
    rims_start(0)

    near_wait(1, cp_recv)
    total = cp_recv[0]
    for slot in range(1, SLOTS // 2 * sections):
        total = total + cp_recv[slot]
    high, low = halves(total)
    embed_high, embed_low = halves(embed[...])
    outer = dot_tn(
        jnp.concatenate([high, low, high], axis=0),
        jnp.concatenate([embed_high, embed_high, embed_low], axis=0),
    )
    mixed[...] = (atm[...].astype(F32) + outer).astype(BF16)
    pack(0, dot(table_t[...], mixed[...]))

    def forward_cells(layer, store):
        def cells(row):
            unit, _ = normalize(hid[layer, row])
            normed = (unit * gains[layer : layer + 1, :]).astype(BF16)
            before = dot(normed, expand[layer])
            _, wave = gelu_parts(before)
            active = gelu_value(before, wave).astype(BF16)
            update = dot(active, project[layer])
            old = wide[row + radius, MARGIN:right, :]
            store(row, (old + mask_wide[row].astype(F32) * update).astype(BF16))

        loop(rows, cells)

    def hidden_store(layer):
        def store(row, begin, value):
            hid[layer, row, pl.ds(begin, 8), :] = value

        return store

    def hidden_base(layer):
        return lambda row, begin: hid[layer, row, pl.ds(begin, 8), :]

    nothing = lambda row, begin: None

    first_part(0, 0, False, nothing, hidden_store(0))
    spectral(0, leg_f, dot, leg_i, dot, False)
    second_part(0, 0, False, hidden_base(0), hidden_store(0))

    def to_window(row, value):
        win[1, row + radius, MARGIN:right, :] = value

    forward_cells(0, to_window)
    rims_start(1)

    all_wait(1)
    response = dot(table[...], unpack(1))
    square, wave = gelu_parts(response)
    atm_next[...] = (mixed[...].astype(F32) + gelu_value(response, wave)).astype(BF16)
    slope = gelu_slope(response, square, wave)
    mixed[...] = (slope * acot[...].astype(F32)).astype(BF16)
    pack(2, dot(table_t[...], mixed[...]))

    first_part(1, 1, False, nothing, hidden_store(1))
    spectral(2, leg_i, dot_tn, leg_f, dot_tn, True)
    second_part(1, 1, False, hidden_base(1), hidden_store(1))

    def backward(layer, row, hidden, cotangent, window):
        gain = gains[layer : layer + 1, :]
        unit, inverse_std = normalize(hidden)
        normed = (unit * gain).astype(BF16)
        before = dot(normed, expand[layer])
        masked = (mask_wide[row].astype(F32) * cotangent).astype(BF16)
        active_adjoint = dot_nt(masked, project[layer])
        square, wave = gelu_parts(before)
        before_adjoint = (gelu_slope(before, square, wave) * active_adjoint).astype(BF16)
        scaled = dot_nt(before_adjoint, expand[layer]) * gain
        adjoint = inverse_std * (
            scaled
            - jnp.mean(scaled, axis=-1, keepdims=True)
            - unit * jnp.mean(scaled * unit, axis=-1, keepdims=True)
        )
        win[window, row + radius, MARGIN:right, :] = adjoint.astype(BF16)
        return before, wave

    def turn(row):
        before, wave = backward(1, row, hid[1, row], ocot[row].astype(F32), 2)
        active = gelu_value(before, wave).astype(BF16)
        update = dot(active, project[1])
        old = wide[row + radius, MARGIN:right, :]
        ocean_next[row] = (old + mask_wide[row].astype(F32) * update).astype(BF16)

    loop(rows, turn)
    rims_start(2)

    all_wait(3)
    acot_wide = acot[...].astype(F32)
    input_adjoint = acot_wide + dot(table[...], unpack(3))
    atm_grad[...] = input_adjoint
    high, low = halves(input_adjoint)
    embed_high, embed_low = halves(embed[...])
    sa_send[...] = (
        dot_nt(embed_high, high) + dot_nt(embed_low, high) + dot_nt(embed_high, low)
    )
    band_to_groups(2, sa_send, sa_recv, start)

    def grad_store(row, begin, value):
        ocean_grad[row, pl.ds(begin, 8), :] = value

    def grad_base(row, begin):
        return ocean_grad[row, pl.ds(begin, 8), :]

    def given(row, begin):
        return ocot[row, pl.ds(begin, 8), :].astype(F32)

    first_part(2, 1, True, given, grad_store)
    second_part(2, 1, True, grad_base, grad_store)

    loop(rows, lambda row: backward(0, row, hid[0, row], ocean_grad[row], 3) and None)
    rims_start(3)

    near_wait(2, sa_recv)
    for row in range(rows):
        total = wa[0, row] * sa_recv[0]
        for slot in range(1, SLOTS):
            total = total + wa[slot, row] * sa_recv[slot]
        surf[row : row + 1, 0:lon] = total
    high, low = halves(surf[:, 0:lon])
    widened = (dot_nt(high, repeat[...]) + dot_nt(low, repeat[...])) * mask_value * (1.0 / ratio)
    surf[...] = widened

    first_part(3, 0, True, grad_base, grad_store)
    second_part(3, 0, True, grad_base, grad_store)

    def fold_row(row):
        masked = (mask_wide[row].astype(F32) * ocean_grad[row]).astype(BF16)
        fold[row] = dot_nt(flux_embed[...], masked)

    loop(rows, fold_row)
    for row in range(rows):
        high, low = halves(fold[row])
        fold[row, :, 0:lon] = dot(high, repeat[...]) + dot(low, repeat[...])

    def flux_part(slot):
        total = wo[slot, 0] * fold[0, :, 0:lon]
        for row in range(1, rows):
            total = total + wo[slot, row] * fold[row, :, 0:lon]
        fa_send[slot] = total

    loop(SLOTS, flux_part)
    group_to_bands(3, fa_send, fa_recv, start)

    read_rows = jnp.concatenate([read[...].astype(F32)] * rows, axis=1)
    block_read = jnp.where(inside, read_rows, 0.0).astype(BF16)
    high, low = halves(surf[...])
    share = dot_tn(high, block_read) + dot_tn(low, block_read)
    for row in range(rows):
        ocean_grad[row] = ocean_grad[row] + share[:, row * LANES : (row + 1) * LANES]

    near_wait(3, fa_recv)
    total = fa_recv[0]
    for slot in range(1, SLOTS // 2 * sections):
        total = total + fa_recv[slot]
    high, low = halves(total)
    rows_read = flux_read_t[...]
    atm_grad[...] = atm_grad[...] + dot_tn(high, rows_read) + dot_tn(low, rows_read)

    band_to_groups(0, flux_send, flux_recv, sent)
    group_to_bands(1, cp_send, cp_recv, sent)
    band_to_groups(2, sa_send, sa_recv, sent)
    group_to_bands(3, fa_send, fa_recv, sent)
    for index in range(xs.shape[0]):
        all_sent(index)
    for layer in range(win.shape[0]):
        rims_sent(layer)


def per_device(
    atmosphere,
    ocean_state,
    land_mask,
    crossing_bands,
    ocean_regrid,
    atmosphere_regrid,
    surface_read,
    surface_embed,
    flux_read,
    flux_embed,
    legendre_forward,
    legendre_inverse,
    spectral_mix,
    conv_kernel,
    norm_gain,
    expand_weight,
    project_weight,
    atmosphere_cotangent,
    ocean_cotangent,
):
    axes = (lax.axis_size("sec"), lax.axis_size("tile"))
    devices = axes[0] * axes[1]
    lat_rows, lon, channels = atmosphere.shape
    rows, extent, ocean_channels = ocean_state.shape
    layers, side = conv_kernel.shape[0], conv_kernel.shape[1]
    fluxes = flux_read.shape[1]
    peers = crossing_bands.shape[1]
    modes, lat_count, _ = legendre_forward.shape
    cols = 2 * modes
    radius = side // 2
    assert lat_rows == 1 and lat_count == devices and devices == 2 * axes[1]
    assert layers == 2 and ocean_channels == LANES and extent % MARGIN == 0
    table = wave_table(lon, modes * devices)
    order = mode_order(lat_count, modes)
    operands = [
        atmosphere[0],
        ocean_state,
        land_mask,
        crossing_bands,
        ocean_regrid.reshape(peers, rows),
        atmosphere_regrid.reshape(peers, rows),
        surface_read[None, :],
        surface_embed[None, :],
        flux_read.T,
        flux_embed,
        legendre_forward,
        legendre_inverse,
        spectral_mix,
        conv_kernel.astype(F32).reshape(layers, side * side, ocean_channels),
        norm_gain,
        expand_weight,
        project_weight,
        atmosphere_cotangent[0],
        ocean_cotangent,
        jnp.asarray(table),
        jnp.asarray(np.ascontiguousarray(table.T)),
        jnp.asarray(order),
        jnp.asarray(np.ascontiguousarray(order.T)),
    ]
    scalars = (3, 4, 5)
    near = SLOTS // 2 * axes[0]
    shape = (rows, extent, ocean_channels)
    outs = (
        jax.ShapeDtypeStruct((lon, channels), BF16),
        jax.ShapeDtypeStruct(shape, BF16),
        jax.ShapeDtypeStruct((lon, channels), F32),
        jax.ShapeDtypeStruct(shape, F32),
    )
    window = (rows + 2 * radius, extent + 2 * MARGIN, ocean_channels)
    block = cols * devices
    vmem = pltpu.VMEM
    results = pl.pallas_call(
        functools.partial(window_kernel, axes),
        out_shape=outs,
        in_specs=[
            pl.BlockSpec(memory_space=pltpu.SMEM if index in scalars else pltpu.VMEM)
            for index in range(len(operands))
        ],
        out_specs=tuple(pl.BlockSpec(memory_space=pltpu.VMEM) for _ in outs),
        scratch_shapes=[
            vmem((2 * layers,) + window, BF16),
            vmem(window, F32),
            vmem((layers,) + shape, F32),
            vmem((layers, side * side, 8, ocean_channels), F32),
            vmem(shape, BF16),
            vmem((extent, lon), BF16),
            vmem((rows, extent), F32),
            vmem((rows, lon, ocean_channels), BF16),
            vmem((rows, fluxes, extent), F32),
            pltpu.SMEM((SLOTS, rows), F32),
            pltpu.SMEM((SLOTS, rows), F32),
            vmem((fluxes, lon), F32),
            vmem((SLOTS, fluxes, lon), F32),
            vmem((SLOTS, 1, lon), F32),
            vmem((near, 1, lon), F32),
            vmem((1, lon), F32),
            vmem((SLOTS, 1, lon), F32),
            vmem((SLOTS, fluxes, lon), F32),
            vmem((near, fluxes, lon), F32),
            vmem((4, devices, cols, channels), BF16),
            vmem((4, devices, cols, channels), BF16),
            vmem((block, channels), F32),
            vmem((lon, channels), BF16),
            vmem((block, channels), BF16),
            vmem((block, channels), BF16),
            pltpu.SemaphoreType.DMA((2 * layers, 8)),
            pltpu.SemaphoreType.DMA((2 * layers, 8)),
            pltpu.SemaphoreType.DMA((4,)),
            pltpu.SemaphoreType.DMA((4,)),
            pltpu.SemaphoreType.DMA((4, SLOTS)),
            pltpu.SemaphoreType.DMA((4,)),
        ],
        compiler_params=pltpu.CompilerParams(
            collective_id=0, has_side_effects=True, vmem_limit_bytes=60 * 1024 * 1024
        ),
    )(*operands)
    atm_next, ocean_next, atm_grad, ocean_grad = results
    return (atm_next[None], ocean_next, atm_grad[None], ocean_grad)


def solution(mesh):
    return jax.shard_map(
        per_device,
        mesh=mesh,
        in_specs=(
            P(("sec", "tile"), None, None),
            P("tile", "sec", None),
            P("tile", "sec"),
            P("tile", None),
            P("tile", None, None, None),
            P("tile", None, None, None),
            P(),
            P(),
            P(),
            P(),
            P(("sec", "tile"), None, None),
            P(("sec", "tile"), None, None),
            P(),
            P(),
            P(),
            P(),
            P(),
            P(("sec", "tile"), None, None),
            P("tile", "sec", None),
        ),
        out_specs=(
            P(("sec", "tile"), None, None),
            P("tile", "sec", None),
            P(("sec", "tile"), None, None),
            P("tile", "sec", None),
        ),
        check_vma=False,
    )
```

```python
import functools

import jax
import jax.numpy as jnp
import numpy as np
from jax import lax
from jax.experimental import pallas as pl
from jax.experimental.pallas import tpu as pltpu
from jax.sharding import PartitionSpec as P

MESH = pl.DeviceIdType.MESH
F32 = jnp.float32
BF16 = jnp.bfloat16
GELU_SCALE = 0.7978845608028654
GELU_CUBIC = 0.044715
EPSILON = 1e-06
MARGIN = 16
SLOTS = 8
LANES = 128
STEP = 16


def wave_table(lon_count, mode_count):
    longitude = np.arange(lon_count)
    wavenumber = np.arange(mode_count)
    phase = (longitude[:, None] * wavenumber[None, :] % lon_count) * (2.0 * np.pi / lon_count)
    scaled = np.stack([np.cos(phase), -np.sin(phase)], axis=2) * np.sqrt(2.0 / lon_count)
    return scaled.reshape(lon_count, 2 * mode_count).astype(np.float32).astype(BF16)


def mode_order(lat_count, modes):
    source = np.arange(lat_count * modes * 2)
    lat, mode, part = source // (2 * modes), source % (2 * modes) // 2, source % 2
    matrix = np.zeros((source.size, source.size), np.float32)
    matrix[(part * modes + mode) * lat_count + lat, source] = 1.0
    return matrix.astype(BF16)


def dot(a, b):
    return lax.dot_general(a, b, (((1,), (0,)), ((), ())), preferred_element_type=F32)


def dot_nt(a, b):
    return lax.dot_general(a, b, (((1,), (1,)), ((), ())), preferred_element_type=F32)


def dot_tn(a, b):
    return lax.dot_general(a, b, (((0,), (0,)), ((), ())), preferred_element_type=F32)


def halves(x):
    high = x.astype(BF16)
    return high, (x - high.astype(F32)).astype(BF16)


def loop(count, body):
    def step(index, carry):
        body(index)
        return carry

    lax.fori_loop(0, count, step, jnp.int32(0))


def normalize(hidden):
    center = hidden - jnp.mean(hidden, axis=-1, keepdims=True)
    inverse_std = lax.rsqrt(jnp.mean(center * center, axis=-1, keepdims=True) + EPSILON)
    return center * inverse_std, inverse_std


def gelu_parts(before):
    square = before * before
    wave = jnp.tanh(before * (GELU_SCALE + (GELU_SCALE * GELU_CUBIC) * square))
    return square, wave


def gelu_value(before, wave):
    scaled = 0.5 * before
    return scaled + scaled * wave


def gelu_slope(before, square, wave):
    slope = (0.5 * GELU_SCALE + (1.5 * GELU_SCALE * GELU_CUBIC) * square) * before
    return 0.5 + 0.5 * wave + slope * (1.0 - wave * wave)


def window_kernel(
    axes,
    atm, ocean, mask, bands, oreg, areg, read, embed, flux_read_t, flux_embed,
    leg_f, leg_i, smix, taps_in, gains, expand, project, acot, ocot,
    table, table_t, order, order_t,
    atm_next, ocean_next, atm_grad, ocean_grad,
    win, wide, hid, taps, mask_wide, repeat, surf, gall, fold,
    wo, wa, flux_send, flux_recv, cp_send, cp_recv, sa_send, sa_recv, fa_send, fa_recv,
    xs, xr, flat, mixed, spec_a, spec_b,
    halo_send, halo_recv, line_send, line_recv, x_send, x_recv, near_send, near_recv,
):
    sections, tiles = axes
    devices = sections * tiles
    sec = lax.axis_index("sec")
    tile = lax.axis_index("tile")
    me = sec * tiles + tile
    rows, extent, channels = ocean.shape
    lon = atm.shape[0]
    radius = (win.shape[1] - rows) // 2
    side = 2 * radius + 1
    part = lon // sections
    ratio = extent // part
    cols = xs.shape[2]
    right = MARGIN + extent

    def target(device):
        return {"sec": lax.div(device, tiles), "tile": lax.rem(device, tiles)}

    barrier = pltpu.get_barrier_semaphore()

    def greet(step):
        pl.semaphore_signal(
            barrier, inc=1, device_id=target(lax.rem(me + 1 + step, devices)), device_id_type=MESH
        )

    loop(devices - 1, greet)

    @pl.when(tile == 0)
    def _():
        win[:, 0:radius] = jnp.zeros((win.shape[0], radius) + win.shape[2:], BF16)

    @pl.when(tile == tiles - 1)
    def _():
        win[:, radius + rows :] = jnp.zeros((win.shape[0], radius) + win.shape[2:], BF16)

    x_index = lax.broadcasted_iota(jnp.int32, (extent, lon), 0)
    g_index = lax.broadcasted_iota(jnp.int32, (extent, lon), 1)
    offset = x_index - (g_index - sec * part) * ratio
    repeat[...] = jnp.where((offset >= 0) & (offset < ratio), 1.0, 0.0).astype(BF16)

    for row in range(rows):
        surf[row : row + 1, :] = dot_nt(read[...], ocean[row])
    mask_value = mask[...].astype(F32)
    high, low = halves(surf[...] * mask_value * (1.0 / ratio))
    surf[:, 0:lon] = dot(high, repeat[...]) + dot(low, repeat[...])

    flux_send[...] = dot_nt(flux_read_t[...], atm[...])

    def weights(slot):
        band = lax.rem(2 * tile - 2 + slot + devices, devices)
        for row in range(rows):
            to_ocean = jnp.float32(0.0)
            to_atm = jnp.float32(0.0)
            for peer in range(bands.shape[1]):
                same = jnp.where(bands[0, peer] == band, 1.0, 0.0)
                to_ocean = to_ocean + same * oreg[peer, row]
                to_atm = to_atm + same * areg[peer, row]
            wo[slot, row] = to_ocean
            wa[slot, row] = to_atm

    loop(SLOTS, weights)

    def coarse_part(slot):
        total = wa[slot, 0] * surf[0:1, 0:lon]
        for row in range(1, rows):
            total = total + wa[slot, row] * surf[row : row + 1, 0:lon]
        cp_send[slot] = total

    loop(SLOTS, coarse_part)

    pl.semaphore_wait(barrier, devices - 1)

    def band_to_groups(index, source, slots, act):
        def one(step):
            turn, section = lax.div(step, sections), lax.rem(step, sections)
            group = lax.rem(lax.div(me, 2) + 1 - turn + tiles, tiles)
            slot = lax.rem(me, 2) + 2 * turn
            away = (section != sec) | (group != tile)

            def remote():
                return pltpu.make_async_remote_copy(
                    src_ref=source,
                    dst_ref=slots.at[slot],
                    send_sem=near_send.at[index, step],
                    recv_sem=near_recv.at[index],
                    device_id={"sec": section, "tile": group},
                    device_id_type=MESH,
                )

            @pl.when(away)
            def _():
                act(remote())

            if act is start:

                @pl.when(jnp.logical_not(away))
                def _():
                    pltpu.make_async_copy(source, slots.at[slot], near_recv.at[index]).start()

        loop(SLOTS // 2 * sections, one)

    def group_to_bands(index, parts, slots, act):
        def one(slot):
            band = lax.rem(2 * tile - 2 + slot + devices, devices)
            place = lax.div(slot, 2) * sections + sec

            def remote():
                return pltpu.make_async_remote_copy(
                    src_ref=parts.at[slot],
                    dst_ref=slots.at[place],
                    send_sem=near_send.at[index, slot],
                    recv_sem=near_recv.at[index],
                    device_id=target(band),
                    device_id_type=MESH,
                )

            @pl.when(band != me)
            def _():
                act(remote())

            if act is start:

                @pl.when(band == me)
                def _():
                    pltpu.make_async_copy(
                        parts.at[slot], slots.at[place], near_recv.at[index]
                    ).start()

        loop(SLOTS, one)

    def start(copy):
        copy.start()

    def sent(copy):
        copy.wait_send()

    def near_wait(index, slots):
        pltpu.make_async_copy(slots, slots, near_recv.at[index]).wait()

    def all_start(index):
        pltpu.make_async_copy(xs.at[index, me], xr.at[index, me], x_recv.at[index]).start()

        def one(step):
            peer = lax.rem(me + 1 + step, devices)
            pltpu.make_async_remote_copy(
                src_ref=xs.at[index, peer],
                dst_ref=xr.at[index, me],
                send_sem=x_send.at[index],
                recv_sem=x_recv.at[index],
                device_id=target(peer),
                device_id_type=MESH,
            ).start()

        loop(devices - 1, one)

    def all_wait(index):
        pltpu.make_async_copy(xr.at[index], xr.at[index], x_recv.at[index]).wait()

    def all_sent(index):
        others = xs.at[index, pl.ds(0, devices - 1)]
        pltpu.make_async_copy(others, others, x_send.at[index]).wait()

    def rim(layer, row_step, col_step):
        number = (row_step + 1) * 3 + col_step + 1
        number = number if number < 4 else number - 1
        source_rows = {-1: (radius, radius), 0: (radius, rows), 1: (rows, radius)}[row_step]
        place_rows = {-1: (radius + rows, radius), 0: (radius, rows), 1: (0, radius)}[row_step]
        inner = {-1: (MARGIN, MARGIN), 0: (MARGIN, extent), 1: (extent, MARGIN)}[col_step]
        outer = {-1: (right, MARGIN), 0: (MARGIN, extent), 1: (0, MARGIN)}[col_step]
        return pltpu.make_async_remote_copy(
            src_ref=win.at[layer, pl.ds(*source_rows), pl.ds(*inner)],
            dst_ref=win.at[layer, pl.ds(*place_rows), pl.ds(*outer)],
            send_sem=halo_send.at[layer, number],
            recv_sem=halo_recv.at[layer, number],
            device_id={
                "sec": lax.rem(sec + col_step + sections, sections),
                "tile": lax.rem(tile + row_step + tiles, tiles),
            },
            device_id_type=MESH,
        )

    def line_copy(layer, row_step, row, number):
        place = row + rows if row_step < 0 else row - rows
        return pltpu.make_async_remote_copy(
            src_ref=win.at[layer, row + radius, pl.ds(MARGIN, extent)],
            dst_ref=win.at[layer, place + radius, pl.ds(MARGIN, extent)],
            send_sem=line_send.at[layer, number],
            recv_sem=line_recv.at[layer, number],
            device_id={"sec": sec, "tile": lax.rem(tile + row_step + tiles, tiles)},
            device_id_type=MESH,
        )

    def line_start(layer, row):
        @pl.when((row < radius) & (tile != 0))
        def _():
            line_copy(layer, -1, row, row).start()

        @pl.when((row >= rows - radius) & (tile != tiles - 1))
        def _():
            line_copy(layer, 1, row, row - (rows - 2 * radius)).start()

    def outer_first(body):
        def one(index):
            half = lax.div(index, 2)
            body(jnp.where(lax.rem(index, 2) == 0, half, rows - 1 - half))

        loop(rows, one)

    def rims(layer, act, line_act, sending, row_steps):
        for row_step in row_steps:
            edge = {-1: 0, 0: None, 1: tiles - 1}[row_step if sending else -row_step]

            def each(row_step=row_step):
                if row_step != 0 and line_act is not None:
                    for step in range(radius):
                        row = step if row_step < 0 else rows - radius + step
                        number = row if row_step < 0 else row - (rows - 2 * radius)
                        line_act(line_copy(layer, row_step, row, number))
                for col_step in (-1, 1):
                    act(rim(layer, row_step, col_step))

            if edge is None:
                each()
            else:
                pl.when(tile != edge)(each)

    def rims_start(layer):
        rims(layer, lambda copy: copy.start(), None, True, (0, -1, 1))

    def rims_sent(layer):
        leave = lambda copy: copy.wait_send()
        rims(layer, leave, leave, True, (0, -1, 1))

    def rims_wait(layer, row_steps):
        arrive = lambda copy: copy.wait_recv()
        rims(layer, arrive, arrive, False, row_steps)

    def widen(layer, first, count):
        def one(index):
            wide[first + index] = win[layer, first + index].astype(F32)

        loop(count, one)

    def depthwise(kernel, flip, lines, base, store):
        def step(index):
            begin = pl.multiple_of(index * STEP, STEP)
            totals = [None] * rows
            for col in range(side):
                tap = [
                    taps[kernel, side * side - 1 - (u * side + col) if flip else u * side + col]
                    for u in range(side)
                ]
                partial = [None] * rows
                for line in lines:
                    piece = wide[line, pl.ds(begin + (MARGIN - radius + col), STEP), :]
                    piece = piece.astype(BF16)
                    for u in range(side):
                        place = line - u
                        if 0 <= place < rows:
                            term = piece * tap[u]
                            old = partial[place]
                            partial[place] = term if old is None else old + term
                for row in range(rows):
                    if partial[row] is not None:
                        value = partial[row].astype(F32)
                        totals[row] = value if totals[row] is None else totals[row] + value
            for row in range(rows):
                if totals[row] is not None:
                    before = base(row, begin)
                    store(row, begin, totals[row] if before is None else before + totals[row])

        loop(extent // STEP, step)

    own_lines = range(radius, radius + rows)
    rim_lines = list(range(radius)) + list(range(radius + rows, rows + 2 * radius))

    def first_part(layer, kernel, flip, base, store):
        rims_wait(layer, (0,))
        widen(layer, radius, rows)
        depthwise(kernel, flip, own_lines, base, store)

    def second_part(layer, kernel, flip, base, store):
        rims_wait(layer, (-1, 1))
        widen(layer, 0, radius)
        widen(layer, radius + rows, radius)
        depthwise(kernel, flip, rim_lines, base, store)

    height = max(cols, 8)
    group = height // cols

    def unpack(index):
        def one(block):
            pieces = [
                xr[index, block * group + place].astype(F32) for place in range(group)
            ]
            flat[pl.ds(pl.multiple_of(block * height, height), height), :] = (
                pieces[0] if group == 1 else jnp.concatenate(pieces, axis=0)
            )

        loop(devices // group, one)
        return flat[...].astype(BF16)

    def pack(index, value):
        flat[...] = value

        def one(block):
            piece = flat[pl.ds(pl.multiple_of(block * height, height), height), :].astype(BF16)
            for place in range(group):
                xs[index, block * group + place] = piece[place * cols : (place + 1) * cols]

        loop(devices // group, one)
        all_start(index)

    def spectral(index, first, first_dot, second, second_dot, adjoint):
        modes, lat = first.shape[0], first.shape[1]
        half = modes * lat
        all_wait(index)
        spec_a[...] = dot(order[...], unpack(index)).astype(BF16)
        for block in range(2 * modes):
            piece = pl.ds(block * lat, lat)
            spec_b[piece] = first_dot(first[block % modes], spec_a[piece]).astype(BF16)
        real, imag = spec_b[0:half], spec_b[half : 2 * half]
        if adjoint:
            spec_a[0:half] = (dot_nt(real, smix[0]) + dot_nt(imag, smix[1])).astype(BF16)
            spec_a[half : 2 * half] = (dot_nt(imag, smix[0]) - dot_nt(real, smix[1])).astype(BF16)
        else:
            spec_a[0:half] = (dot(real, smix[0]) - dot(imag, smix[1])).astype(BF16)
            spec_a[half : 2 * half] = (dot(imag, smix[0]) + dot(real, smix[1])).astype(BF16)
        for block in range(2 * modes):
            piece = pl.ds(block * lat, lat)
            spec_b[piece] = second_dot(second[block % modes], spec_a[piece]).astype(BF16)
        pack(index + 1, dot(order_t[...], spec_b[...]))

    band_to_groups(0, flux_send, flux_recv, start)
    group_to_bands(1, cp_send, cp_recv, start)

    lane_row = lax.broadcasted_iota(jnp.int32, (rows, rows * LANES), 1)
    sub_row = lax.broadcasted_iota(jnp.int32, (rows, rows * LANES), 0)
    inside = (lane_row >= sub_row * LANES) & (lane_row < (sub_row + 1) * LANES)
    spread = jnp.where(inside, 1.0, 0.0).astype(BF16)
    column = dot_tn(mask_value.astype(BF16), spread)
    for row in range(rows):
        mask_wide[row] = column[:, row * LANES : (row + 1) * LANES].astype(BF16)

    def tap_tile(index):
        for kernel in range(taps.shape[0]):
            taps[kernel, index] = jnp.broadcast_to(
                taps_in[kernel, pl.ds(index, 1), :], (STEP, channels)
            ).astype(BF16)

    loop(side * side, tap_tile)

    near_wait(0, flux_recv)
    for row in range(rows):
        total = wo[0, row] * flux_recv[0]
        for slot in range(1, SLOTS):
            total = total + wo[slot, row] * flux_recv[slot]
        high, low = halves(total)
        embed_rows = flux_embed[...]
        gall[row] = (dot_tn(high, embed_rows) + dot_tn(low, embed_rows)).astype(BF16)

    def force(row):
        forcing = dot(repeat[...], gall[row])
        state = ocean[row].astype(F32) + mask_wide[row].astype(F32) * forcing
        win[0, row + radius, MARGIN:right, :] = state.astype(BF16)
        line_start(0, row)

    outer_first(force)
    rims_start(0)

    near_wait(1, cp_recv)
    total = cp_recv[0]
    for slot in range(1, SLOTS // 2 * sections):
        total = total + cp_recv[slot]
    high, low = halves(total)
    embed_high, embed_low = halves(embed[...])
    outer = dot_tn(
        jnp.concatenate([high, low, high], axis=0),
        jnp.concatenate([embed_high, embed_high, embed_low], axis=0),
    )
    mixed[...] = (atm[...].astype(F32) + outer).astype(BF16)
    pack(0, dot(table_t[...], mixed[...]))

    def forward_cells(layer, store):
        def cells(row):
            unit, _ = normalize(hid[layer, row])
            normed = (unit * gains[layer : layer + 1, :]).astype(BF16)
            before = dot(normed, expand[layer])
            _, wave = gelu_parts(before)
            active = gelu_value(before, wave).astype(BF16)
            update = dot(active, project[layer])
            old = wide[row + radius, MARGIN:right, :]
            store(row, (old + mask_wide[row].astype(F32) * update).astype(BF16))

        outer_first(cells)

    def hidden_store(layer):
        def store(row, begin, value):
            hid[layer, row, pl.ds(begin, STEP), :] = value

        return store

    def hidden_base(layer):
        return lambda row, begin: hid[layer, row, pl.ds(begin, STEP), :]

    nothing = lambda row, begin: None

    first_part(0, 0, False, nothing, hidden_store(0))
    spectral(0, leg_f, dot, leg_i, dot, False)
    second_part(0, 0, False, hidden_base(0), hidden_store(0))

    def to_window(row, value):
        win[1, row + radius, MARGIN:right, :] = value
        line_start(1, row)

    forward_cells(0, to_window)
    rims_start(1)

    all_wait(1)
    response = dot(table[...], unpack(1))
    square, wave = gelu_parts(response)
    atm_next[...] = (mixed[...].astype(F32) + gelu_value(response, wave)).astype(BF16)
    slope = gelu_slope(response, square, wave)
    mixed[...] = (slope * acot[...].astype(F32)).astype(BF16)
    pack(2, dot(table_t[...], mixed[...]))

    first_part(1, 1, False, nothing, hidden_store(1))
    spectral(2, leg_i, dot_tn, leg_f, dot_tn, True)
    second_part(1, 1, False, hidden_base(1), hidden_store(1))

    def backward(layer, row, hidden, cotangent, window):
        gain = gains[layer : layer + 1, :]
        unit, inverse_std = normalize(hidden)
        normed = (unit * gain).astype(BF16)
        before = dot(normed, expand[layer])
        masked = (mask_wide[row].astype(F32) * cotangent).astype(BF16)
        active_adjoint = dot_nt(masked, project[layer])
        square, wave = gelu_parts(before)
        before_adjoint = (gelu_slope(before, square, wave) * active_adjoint).astype(BF16)
        scaled = dot_nt(before_adjoint, expand[layer]) * gain
        adjoint = inverse_std * (
            scaled
            - jnp.mean(scaled, axis=-1, keepdims=True)
            - unit * jnp.mean(scaled * unit, axis=-1, keepdims=True)
        )
        win[window, row + radius, MARGIN:right, :] = adjoint.astype(BF16)
        line_start(window, row)
        return before, wave

    def turn(row):
        before, wave = backward(1, row, hid[1, row], ocot[row].astype(F32), 2)
        active = gelu_value(before, wave).astype(BF16)
        update = dot(active, project[1])
        old = wide[row + radius, MARGIN:right, :]
        ocean_next[row] = (old + mask_wide[row].astype(F32) * update).astype(BF16)

    outer_first(turn)
    rims_start(2)

    all_wait(3)
    acot_wide = acot[...].astype(F32)
    input_adjoint = acot_wide + dot(table[...], unpack(3))
    atm_grad[...] = input_adjoint
    high, low = halves(input_adjoint)
    embed_high, embed_low = halves(embed[...])
    sa_send[...] = (
        dot_nt(embed_high, high) + dot_nt(embed_low, high) + dot_nt(embed_high, low)
    )
    band_to_groups(2, sa_send, sa_recv, start)

    def grad_store(row, begin, value):
        ocean_grad[row, pl.ds(begin, STEP), :] = value

    def grad_base(row, begin):
        return ocean_grad[row, pl.ds(begin, STEP), :]

    def given(row, begin):
        return ocot[row, pl.ds(begin, STEP), :].astype(F32)

    first_part(2, 1, True, given, grad_store)
    second_part(2, 1, True, grad_base, grad_store)

    outer_first(lambda row: backward(0, row, hid[0, row], ocean_grad[row], 3) and None)
    rims_start(3)

    near_wait(2, sa_recv)
    for row in range(rows):
        total = wa[0, row] * sa_recv[0]
        for slot in range(1, SLOTS):
            total = total + wa[slot, row] * sa_recv[slot]
        surf[row : row + 1, 0:lon] = total
    high, low = halves(surf[:, 0:lon])
    widened = (dot_nt(high, repeat[...]) + dot_nt(low, repeat[...])) * mask_value * (1.0 / ratio)
    surf[...] = widened

    first_part(3, 0, True, grad_base, grad_store)
    second_part(3, 0, True, grad_base, grad_store)

    def fold_row(row):
        masked = (mask_wide[row].astype(F32) * ocean_grad[row]).astype(BF16)
        fold[row] = dot_nt(flux_embed[...], masked)

    loop(rows, fold_row)
    for row in range(rows):
        high, low = halves(fold[row])
        fold[row, :, 0:lon] = dot(high, repeat[...]) + dot(low, repeat[...])

    def flux_part(slot):
        total = wo[slot, 0] * fold[0, :, 0:lon]
        for row in range(1, rows):
            total = total + wo[slot, row] * fold[row, :, 0:lon]
        fa_send[slot] = total

    loop(SLOTS, flux_part)
    group_to_bands(3, fa_send, fa_recv, start)

    read_rows = jnp.concatenate([read[...].astype(F32)] * rows, axis=1)
    block_read = jnp.where(inside, read_rows, 0.0).astype(BF16)
    high, low = halves(surf[...])
    share = dot_tn(high, block_read) + dot_tn(low, block_read)
    for row in range(rows):
        ocean_grad[row] = ocean_grad[row] + share[:, row * LANES : (row + 1) * LANES]

    near_wait(3, fa_recv)
    total = fa_recv[0]
    for slot in range(1, SLOTS // 2 * sections):
        total = total + fa_recv[slot]
    high, low = halves(total)
    rows_read = flux_read_t[...]
    atm_grad[...] = atm_grad[...] + dot_tn(high, rows_read) + dot_tn(low, rows_read)

    band_to_groups(0, flux_send, flux_recv, sent)
    group_to_bands(1, cp_send, cp_recv, sent)
    band_to_groups(2, sa_send, sa_recv, sent)
    group_to_bands(3, fa_send, fa_recv, sent)
    for index in range(xs.shape[0]):
        all_sent(index)
    for layer in range(win.shape[0]):
        rims_sent(layer)


def per_device(
    atmosphere,
    ocean_state,
    land_mask,
    crossing_bands,
    ocean_regrid,
    atmosphere_regrid,
    surface_read,
    surface_embed,
    flux_read,
    flux_embed,
    legendre_forward,
    legendre_inverse,
    spectral_mix,
    conv_kernel,
    norm_gain,
    expand_weight,
    project_weight,
    atmosphere_cotangent,
    ocean_cotangent,
):
    axes = (lax.axis_size("sec"), lax.axis_size("tile"))
    devices = axes[0] * axes[1]
    lat_rows, lon, channels = atmosphere.shape
    rows, extent, ocean_channels = ocean_state.shape
    layers, side = conv_kernel.shape[0], conv_kernel.shape[1]
    fluxes = flux_read.shape[1]
    peers = crossing_bands.shape[1]
    modes, lat_count, _ = legendre_forward.shape
    cols = 2 * modes
    radius = side // 2
    assert lat_rows == 1 and lat_count == devices and devices == 2 * axes[1]
    assert layers == 2 and ocean_channels == LANES and extent % MARGIN == 0
    table = wave_table(lon, modes * devices)
    order = mode_order(lat_count, modes)
    operands = [
        atmosphere[0],
        ocean_state,
        land_mask,
        crossing_bands,
        ocean_regrid.reshape(peers, rows),
        atmosphere_regrid.reshape(peers, rows),
        surface_read[None, :],
        surface_embed[None, :],
        flux_read.T,
        flux_embed,
        legendre_forward,
        legendre_inverse,
        spectral_mix,
        conv_kernel.astype(F32).reshape(layers, side * side, ocean_channels),
        norm_gain,
        expand_weight,
        project_weight,
        atmosphere_cotangent[0],
        ocean_cotangent,
        jnp.asarray(table),
        jnp.asarray(np.ascontiguousarray(table.T)),
        jnp.asarray(order),
        jnp.asarray(np.ascontiguousarray(order.T)),
    ]
    scalars = (3, 4, 5)
    near = SLOTS // 2 * axes[0]
    shape = (rows, extent, ocean_channels)
    outs = (
        jax.ShapeDtypeStruct((lon, channels), BF16),
        jax.ShapeDtypeStruct(shape, BF16),
        jax.ShapeDtypeStruct((lon, channels), F32),
        jax.ShapeDtypeStruct(shape, F32),
    )
    window = (rows + 2 * radius, extent + 2 * MARGIN, ocean_channels)
    block = cols * devices
    vmem = pltpu.VMEM
    results = pl.pallas_call(
        functools.partial(window_kernel, axes),
        out_shape=outs,
        in_specs=[
            pl.BlockSpec(memory_space=pltpu.SMEM if index in scalars else pltpu.VMEM)
            for index in range(len(operands))
        ],
        out_specs=tuple(pl.BlockSpec(memory_space=pltpu.VMEM) for _ in outs),
        scratch_shapes=[
            vmem((2 * layers,) + window, BF16),
            vmem(window, F32),
            vmem((layers,) + shape, F32),
            vmem((layers, side * side, STEP, ocean_channels), BF16),
            vmem(shape, BF16),
            vmem((extent, lon), BF16),
            vmem((rows, extent), F32),
            vmem((rows, lon, ocean_channels), BF16),
            vmem((rows, fluxes, extent), F32),
            pltpu.SMEM((SLOTS, rows), F32),
            pltpu.SMEM((SLOTS, rows), F32),
            vmem((fluxes, lon), F32),
            vmem((SLOTS, fluxes, lon), F32),
            vmem((SLOTS, 1, lon), F32),
            vmem((near, 1, lon), F32),
            vmem((1, lon), F32),
            vmem((SLOTS, 1, lon), F32),
            vmem((SLOTS, fluxes, lon), F32),
            vmem((near, fluxes, lon), F32),
            vmem((4, devices, cols, channels), BF16),
            vmem((4, devices, cols, channels), BF16),
            vmem((block, channels), F32),
            vmem((lon, channels), BF16),
            vmem((block, channels), BF16),
            vmem((block, channels), BF16),
            pltpu.SemaphoreType.DMA((2 * layers, 8)),
            pltpu.SemaphoreType.DMA((2 * layers, 8)),
            pltpu.SemaphoreType.DMA((2 * layers, 2 * radius)),
            pltpu.SemaphoreType.DMA((2 * layers, 2 * radius)),
            pltpu.SemaphoreType.DMA((4,)),
            pltpu.SemaphoreType.DMA((4,)),
            pltpu.SemaphoreType.DMA((4, SLOTS)),
            pltpu.SemaphoreType.DMA((4,)),
        ],
        compiler_params=pltpu.CompilerParams(
            collective_id=0, has_side_effects=True, vmem_limit_bytes=60 * 1024 * 1024
        ),
    )(*operands)
    atm_next, ocean_next, atm_grad, ocean_grad = results
    return (atm_next[None], ocean_next, atm_grad[None], ocean_grad)


def solution(mesh):
    return jax.shard_map(
        per_device,
        mesh=mesh,
        in_specs=(
            P(("sec", "tile"), None, None),
            P("tile", "sec", None),
            P("tile", "sec"),
            P("tile", None),
            P("tile", None, None, None),
            P("tile", None, None, None),
            P(),
            P(),
            P(),
            P(),
            P(("sec", "tile"), None, None),
            P(("sec", "tile"), None, None),
            P(),
            P(),
            P(),
            P(),
            P(),
            P(("sec", "tile"), None, None),
            P("tile", "sec", None),
        ),
        out_specs=(
            P(("sec", "tile"), None, None),
            P("tile", "sec", None),
            P(("sec", "tile"), None, None),
            P("tile", "sec", None),
        ),
        check_vma=False,
    )
```

```python
import functools

import jax
import jax.numpy as jnp
import numpy as np
from jax import lax
from jax.experimental import pallas as pl
from jax.experimental.pallas import tpu as pltpu
from jax.sharding import PartitionSpec as P

MESH = pl.DeviceIdType.MESH
F32 = jnp.float32
BF16 = jnp.bfloat16
GELU_SCALE = 0.7978845608028654
GELU_CUBIC = 0.044715
EPSILON = 1e-06
MARGIN = 16
SLOTS = 8
LANES = 128
STEP = 16


def wave_table(lon_count, mode_count):
    longitude = np.arange(lon_count)
    wavenumber = np.arange(mode_count)
    phase = (longitude[:, None] * wavenumber[None, :] % lon_count) * (2.0 * np.pi / lon_count)
    scaled = np.stack([np.cos(phase), -np.sin(phase)], axis=2) * np.sqrt(2.0 / lon_count)
    return scaled.reshape(lon_count, 2 * mode_count).astype(np.float32).astype(BF16)


def mode_order(lat_count, modes):
    source = np.arange(lat_count * modes * 2)
    lat, mode, part = source // (2 * modes), source % (2 * modes) // 2, source % 2
    matrix = np.zeros((source.size, source.size), np.float32)
    matrix[(part * modes + mode) * lat_count + lat, source] = 1.0
    return matrix.astype(BF16)


def dot(a, b):
    return lax.dot_general(a, b, (((1,), (0,)), ((), ())), preferred_element_type=F32)


def dot_nt(a, b):
    return lax.dot_general(a, b, (((1,), (1,)), ((), ())), preferred_element_type=F32)


def dot_tn(a, b):
    return lax.dot_general(a, b, (((0,), (0,)), ((), ())), preferred_element_type=F32)


def halves(x):
    high = x.astype(BF16)
    return high, (x - high.astype(F32)).astype(BF16)


def loop(count, body):
    def step(index, carry):
        body(index)
        return carry

    lax.fori_loop(0, count, step, jnp.int32(0))


def normalize(hidden):
    center = hidden - jnp.mean(hidden, axis=-1, keepdims=True)
    inverse_std = lax.rsqrt(jnp.mean(center * center, axis=-1, keepdims=True) + EPSILON)
    return center * inverse_std, inverse_std


def gelu_parts(before):
    square = before * before
    wave = jnp.tanh(before * (GELU_SCALE + (GELU_SCALE * GELU_CUBIC) * square))
    return square, wave


def gelu_value(before, wave):
    scaled = 0.5 * before
    return scaled + scaled * wave


def gelu_slope(before, square, wave):
    slope = (0.5 * GELU_SCALE + (1.5 * GELU_SCALE * GELU_CUBIC) * square) * before
    return (1.0 + wave) * (0.5 + slope * (1.0 - wave))


def window_kernel(
    axes,
    atm, ocean, mask, bands, oreg, areg, read, embed, flux_read_t, flux_embed,
    leg_f, leg_i, smix, taps_in, gains, expand, project, acot, ocot,
    table, table_t, order, order_t,
    atm_next, ocean_next, atm_grad, ocean_grad,
    win, wide, hid, taps, mask_wide, repeat, surf, gall, fold,
    wo, wa, flux_send, flux_recv, cp_send, cp_recv, sa_send, sa_recv, fa_send, fa_recv,
    xs, xr, flat, mixed, spec_a, spec_b,
    halo_send, halo_recv, line_send, line_recv, x_send, x_recv, near_send, near_recv,
):
    sections, tiles = axes
    devices = sections * tiles
    sec = lax.axis_index("sec")
    tile = lax.axis_index("tile")
    me = sec * tiles + tile
    rows, extent, channels = ocean.shape
    lon = atm.shape[0]
    radius = (win.shape[1] - rows) // 2
    side = 2 * radius + 1
    part = lon // sections
    ratio = extent // part
    cols = xs.shape[2]
    right = MARGIN + extent

    def target(device):
        return {"sec": lax.div(device, tiles), "tile": lax.rem(device, tiles)}

    barrier = pltpu.get_barrier_semaphore()

    def greet(step):
        pl.semaphore_signal(
            barrier, inc=1, device_id=target(lax.rem(me + 1 + step, devices)), device_id_type=MESH
        )

    loop(devices - 1, greet)

    @pl.when(tile == 0)
    def _():
        win[:, 0:radius] = jnp.zeros((win.shape[0], radius) + win.shape[2:], BF16)

    @pl.when(tile == tiles - 1)
    def _():
        win[:, radius + rows :] = jnp.zeros((win.shape[0], radius) + win.shape[2:], BF16)

    x_index = lax.broadcasted_iota(jnp.int32, (extent, lon), 0)
    g_index = lax.broadcasted_iota(jnp.int32, (extent, lon), 1)
    offset = x_index - (g_index - sec * part) * ratio
    repeat[...] = jnp.where((offset >= 0) & (offset < ratio), 1.0, 0.0).astype(BF16)

    for row in range(rows):
        surf[row : row + 1, :] = dot_nt(read[...], ocean[row])
    mask_value = mask[...].astype(F32)
    high, low = halves(surf[...] * mask_value * (1.0 / ratio))
    surf[:, 0:lon] = dot(high, repeat[...]) + dot(low, repeat[...])

    flux_send[...] = dot_nt(flux_read_t[...], atm[...])

    def weights(slot):
        band = lax.rem(2 * tile - 2 + slot + devices, devices)
        for row in range(rows):
            to_ocean = jnp.float32(0.0)
            to_atm = jnp.float32(0.0)
            for peer in range(bands.shape[1]):
                same = jnp.where(bands[0, peer] == band, 1.0, 0.0)
                to_ocean = to_ocean + same * oreg[peer, row]
                to_atm = to_atm + same * areg[peer, row]
            wo[slot, row] = to_ocean
            wa[slot, row] = to_atm

    loop(SLOTS, weights)

    def coarse_part(slot):
        total = wa[slot, 0] * surf[0:1, 0:lon]
        for row in range(1, rows):
            total = total + wa[slot, row] * surf[row : row + 1, 0:lon]
        cp_send[slot] = total

    loop(SLOTS, coarse_part)

    pl.semaphore_wait(barrier, devices - 1)

    def band_to_groups(index, source, slots, act):
        def one(step):
            turn, section = lax.div(step, sections), lax.rem(step, sections)
            group = lax.rem(lax.div(me, 2) + 1 - turn + tiles, tiles)
            slot = lax.rem(me, 2) + 2 * turn
            away = (section != sec) | (group != tile)

            def remote():
                return pltpu.make_async_remote_copy(
                    src_ref=source,
                    dst_ref=slots.at[slot],
                    send_sem=near_send.at[index, step],
                    recv_sem=near_recv.at[index],
                    device_id={"sec": section, "tile": group},
                    device_id_type=MESH,
                )

            @pl.when(away)
            def _():
                act(remote())

            if act is start:

                @pl.when(jnp.logical_not(away))
                def _():
                    pltpu.make_async_copy(source, slots.at[slot], near_recv.at[index]).start()

        loop(SLOTS // 2 * sections, one)

    def group_to_bands(index, parts, slots, act):
        def one(slot):
            band = lax.rem(2 * tile - 2 + slot + devices, devices)
            place = lax.div(slot, 2) * sections + sec

            def remote():
                return pltpu.make_async_remote_copy(
                    src_ref=parts.at[slot],
                    dst_ref=slots.at[place],
                    send_sem=near_send.at[index, slot],
                    recv_sem=near_recv.at[index],
                    device_id=target(band),
                    device_id_type=MESH,
                )

            @pl.when(band != me)
            def _():
                act(remote())

            if act is start:

                @pl.when(band == me)
                def _():
                    pltpu.make_async_copy(
                        parts.at[slot], slots.at[place], near_recv.at[index]
                    ).start()

        loop(SLOTS, one)

    def start(copy):
        copy.start()

    def sent(copy):
        copy.wait_send()

    def near_wait(index, slots):
        pltpu.make_async_copy(slots, slots, near_recv.at[index]).wait()

    def all_start(index):
        pltpu.make_async_copy(xs.at[index, me], xr.at[index, me], x_recv.at[index]).start()

        def one(step):
            peer = lax.rem(me + 1 + step, devices)
            pltpu.make_async_remote_copy(
                src_ref=xs.at[index, peer],
                dst_ref=xr.at[index, me],
                send_sem=x_send.at[index],
                recv_sem=x_recv.at[index],
                device_id=target(peer),
                device_id_type=MESH,
            ).start()

        loop(devices - 1, one)

    def all_wait(index):
        pltpu.make_async_copy(xr.at[index], xr.at[index], x_recv.at[index]).wait()

    def all_sent(index):
        others = xs.at[index, pl.ds(0, devices - 1)]
        pltpu.make_async_copy(others, others, x_send.at[index]).wait()

    def rim(layer, row_step, col_step):
        number = (row_step + 1) * 3 + col_step + 1
        number = number if number < 4 else number - 1
        source_rows = {-1: (radius, radius), 0: (radius, rows), 1: (rows, radius)}[row_step]
        place_rows = {-1: (radius + rows, radius), 0: (radius, rows), 1: (0, radius)}[row_step]
        inner = {-1: (MARGIN, MARGIN), 0: (MARGIN, extent), 1: (extent, MARGIN)}[col_step]
        outer = {-1: (right, MARGIN), 0: (MARGIN, extent), 1: (0, MARGIN)}[col_step]
        return pltpu.make_async_remote_copy(
            src_ref=win.at[layer, pl.ds(*source_rows), pl.ds(*inner)],
            dst_ref=win.at[layer, pl.ds(*place_rows), pl.ds(*outer)],
            send_sem=halo_send.at[layer, number],
            recv_sem=halo_recv.at[layer, number],
            device_id={
                "sec": lax.rem(sec + col_step + sections, sections),
                "tile": lax.rem(tile + row_step + tiles, tiles),
            },
            device_id_type=MESH,
        )

    def line_copy(layer, row_step, row, number):
        place = row + rows if row_step < 0 else row - rows
        return pltpu.make_async_remote_copy(
            src_ref=win.at[layer, row + radius, pl.ds(MARGIN, extent)],
            dst_ref=win.at[layer, place + radius, pl.ds(MARGIN, extent)],
            send_sem=line_send.at[layer, number],
            recv_sem=line_recv.at[layer, number],
            device_id={"sec": sec, "tile": lax.rem(tile + row_step + tiles, tiles)},
            device_id_type=MESH,
        )

    def line_start(layer, row):
        @pl.when((row < radius) & (tile != 0))
        def _():
            line_copy(layer, -1, row, row).start()

        @pl.when((row >= rows - radius) & (tile != tiles - 1))
        def _():
            line_copy(layer, 1, row, row - (rows - 2 * radius)).start()

    def outer_first(body):
        def one(index):
            half = lax.div(index, 2)
            body(jnp.where(lax.rem(index, 2) == 0, half, rows - 1 - half))

        loop(rows, one)

    def rims(layer, act, line_act, sending, row_steps):
        for row_step in row_steps:
            edge = {-1: 0, 0: None, 1: tiles - 1}[row_step if sending else -row_step]

            def each(row_step=row_step):
                if row_step != 0 and line_act is not None:
                    for step in range(radius):
                        row = step if row_step < 0 else rows - radius + step
                        number = row if row_step < 0 else row - (rows - 2 * radius)
                        line_act(line_copy(layer, row_step, row, number))
                for col_step in (-1, 1):
                    act(rim(layer, row_step, col_step))

            if edge is None:
                each()
            else:
                pl.when(tile != edge)(each)

    def rims_start(layer):
        rims(layer, lambda copy: copy.start(), None, True, (0, -1, 1))

    def rims_sent(layer):
        leave = lambda copy: copy.wait_send()
        rims(layer, leave, leave, True, (0, -1, 1))

    def rims_wait(layer, row_steps):
        arrive = lambda copy: copy.wait_recv()
        rims(layer, arrive, arrive, False, row_steps)

    def widen(layer, first, count):
        def one(index):
            wide[first + index] = win[layer, first + index].astype(F32)

        loop(count, one)

    def depthwise(kernel, flip, lines, base, store):
        def step(index):
            begin = pl.multiple_of(index * STEP, STEP)
            totals = [None] * rows
            for col in range(side):
                tap = [
                    taps[kernel, side * side - 1 - (u * side + col) if flip else u * side + col]
                    for u in range(side)
                ]
                partial = [None] * rows
                for line in lines:
                    piece = wide[line, pl.ds(begin + (MARGIN - radius + col), STEP), :]
                    piece = piece.astype(BF16)
                    for u in range(side):
                        place = line - u
                        if 0 <= place < rows:
                            term = piece * tap[u]
                            old = partial[place]
                            partial[place] = term if old is None else old + term
                for row in range(rows):
                    if partial[row] is not None:
                        value = partial[row].astype(F32)
                        totals[row] = value if totals[row] is None else totals[row] + value
            for row in range(rows):
                if totals[row] is not None:
                    before = base(row, begin)
                    store(row, begin, totals[row] if before is None else before + totals[row])

        loop(extent // STEP, step)

    own_lines = range(radius, radius + rows)
    rim_lines = list(range(radius)) + list(range(radius + rows, rows + 2 * radius))

    def first_part(layer, kernel, flip, base, store):
        rims_wait(layer, (0,))
        widen(layer, radius, rows)
        depthwise(kernel, flip, own_lines, base, store)

    def second_part(layer, kernel, flip, base, store):
        rims_wait(layer, (-1, 1))
        widen(layer, 0, radius)
        widen(layer, radius + rows, radius)
        depthwise(kernel, flip, rim_lines, base, store)

    height = max(cols, 8)
    group = height // cols

    def unpack(index):
        def one(block):
            pieces = [
                xr[index, block * group + place].astype(F32) for place in range(group)
            ]
            flat[pl.ds(pl.multiple_of(block * height, height), height), :] = (
                pieces[0] if group == 1 else jnp.concatenate(pieces, axis=0)
            )

        loop(devices // group, one)
        return flat[...].astype(BF16)

    def pack(index, value):
        flat[...] = value

        def one(block):
            piece = flat[pl.ds(pl.multiple_of(block * height, height), height), :].astype(BF16)
            for place in range(group):
                xs[index, block * group + place] = piece[place * cols : (place + 1) * cols]

        loop(devices // group, one)
        all_start(index)

    def spectral(index, first, first_dot, second, second_dot, adjoint):
        modes, lat = first.shape[0], first.shape[1]
        half = modes * lat
        all_wait(index)
        spec_a[...] = dot(order[...], unpack(index)).astype(BF16)
        for block in range(2 * modes):
            piece = pl.ds(block * lat, lat)
            spec_b[piece] = first_dot(first[block % modes], spec_a[piece]).astype(BF16)
        real, imag = spec_b[0:half], spec_b[half : 2 * half]
        if adjoint:
            spec_a[0:half] = (dot_nt(real, smix[0]) + dot_nt(imag, smix[1])).astype(BF16)
            spec_a[half : 2 * half] = (dot_nt(imag, smix[0]) - dot_nt(real, smix[1])).astype(BF16)
        else:
            spec_a[0:half] = (dot(real, smix[0]) - dot(imag, smix[1])).astype(BF16)
            spec_a[half : 2 * half] = (dot(imag, smix[0]) + dot(real, smix[1])).astype(BF16)
        for block in range(2 * modes):
            piece = pl.ds(block * lat, lat)
            spec_b[piece] = second_dot(second[block % modes], spec_a[piece]).astype(BF16)
        pack(index + 1, dot(order_t[...], spec_b[...]))

    band_to_groups(0, flux_send, flux_recv, start)
    group_to_bands(1, cp_send, cp_recv, start)

    lane_row = lax.broadcasted_iota(jnp.int32, (rows, rows * LANES), 1)
    sub_row = lax.broadcasted_iota(jnp.int32, (rows, rows * LANES), 0)
    inside = (lane_row >= sub_row * LANES) & (lane_row < (sub_row + 1) * LANES)
    spread = jnp.where(inside, 1.0, 0.0).astype(BF16)
    column = dot_tn(mask_value.astype(BF16), spread)
    for row in range(rows):
        mask_wide[row] = column[:, row * LANES : (row + 1) * LANES].astype(BF16)

    for kernel in range(taps.shape[0]):
        for u in range(side):
            for v in range(side):
                tile_of = jnp.broadcast_to(taps_in[kernel, u, v : v + 1, :], (STEP, channels))
                taps[kernel, u * side + v] = tile_of.astype(BF16)

    near_wait(0, flux_recv)
    for row in range(rows):
        total = wo[0, row] * flux_recv[0]
        for slot in range(1, SLOTS):
            total = total + wo[slot, row] * flux_recv[slot]
        high, low = halves(total)
        embed_rows = flux_embed[...]
        gall[row] = (dot_tn(high, embed_rows) + dot_tn(low, embed_rows)).astype(BF16)

    def force(row):
        forcing = dot(repeat[...], gall[row])
        state = ocean[row].astype(F32) + mask_wide[row].astype(F32) * forcing
        win[0, row + radius, MARGIN:right, :] = state.astype(BF16)
        line_start(0, row)

    outer_first(force)
    rims_start(0)

    near_wait(1, cp_recv)
    total = cp_recv[0]
    for slot in range(1, SLOTS // 2 * sections):
        total = total + cp_recv[slot]
    high, low = halves(total)
    embed_high, embed_low = halves(embed[...])
    outer = dot_tn(
        jnp.concatenate([high, low, high], axis=0),
        jnp.concatenate([embed_high, embed_high, embed_low], axis=0),
    )
    mixed[...] = (atm[...].astype(F32) + outer).astype(BF16)
    pack(0, dot(table_t[...], mixed[...]))

    def forward_cells(layer, store):
        def cells(row):
            unit, _ = normalize(hid[layer, row])
            normed = (unit * gains[layer : layer + 1, :]).astype(BF16)
            before = dot(normed, expand[layer]).astype(BF16)
            _, wave = gelu_parts(before)
            active = gelu_value(before, wave)
            update = dot(active, project[layer])
            old = wide[row + radius, MARGIN:right, :]
            store(row, (old + mask_wide[row].astype(F32) * update).astype(BF16))

        outer_first(cells)

    def hidden_store(layer):
        def store(row, begin, value):
            hid[layer, row, pl.ds(begin, STEP), :] = value

        return store

    def hidden_base(layer):
        return lambda row, begin: hid[layer, row, pl.ds(begin, STEP), :]

    nothing = lambda row, begin: None

    first_part(0, 0, False, nothing, hidden_store(0))
    spectral(0, leg_f, dot, leg_i, dot, False)
    second_part(0, 0, False, hidden_base(0), hidden_store(0))

    def to_window(row, value):
        win[1, row + radius, MARGIN:right, :] = value
        line_start(1, row)

    forward_cells(0, to_window)
    rims_start(1)

    all_wait(1)
    response = dot(table[...], unpack(1))
    square, wave = gelu_parts(response)
    atm_next[...] = (mixed[...].astype(F32) + gelu_value(response, wave)).astype(BF16)
    slope = gelu_slope(response, square, wave)
    mixed[...] = (slope * acot[...].astype(F32)).astype(BF16)
    pack(2, dot(table_t[...], mixed[...]))

    first_part(1, 1, False, nothing, hidden_store(1))
    spectral(2, leg_i, dot_tn, leg_f, dot_tn, True)
    second_part(1, 1, False, hidden_base(1), hidden_store(1))

    def backward(layer, row, hidden, cotangent, window):
        gain = gains[layer : layer + 1, :]
        unit, inverse_std = normalize(hidden)
        normed = (unit * gain).astype(BF16)
        before = dot(normed, expand[layer]).astype(BF16)
        masked = (mask_wide[row].astype(F32) * cotangent).astype(BF16)
        active_adjoint = dot_nt(masked, project[layer]).astype(BF16)
        square, wave = gelu_parts(before)
        before_adjoint = gelu_slope(before, square, wave) * active_adjoint
        scaled = dot_nt(before_adjoint, expand[layer]) * gain
        adjoint = inverse_std * (
            scaled
            - jnp.mean(scaled, axis=-1, keepdims=True)
            - unit * jnp.mean(scaled * unit, axis=-1, keepdims=True)
        )
        win[window, row + radius, MARGIN:right, :] = adjoint.astype(BF16)
        line_start(window, row)
        return before, wave

    def turn(row):
        before, wave = backward(1, row, hid[1, row], ocot[row].astype(F32), 2)
        active = gelu_value(before, wave)
        update = dot(active, project[1])
        old = wide[row + radius, MARGIN:right, :]
        ocean_next[row] = (old + mask_wide[row].astype(F32) * update).astype(BF16)

    outer_first(turn)
    rims_start(2)

    all_wait(3)
    acot_wide = acot[...].astype(F32)
    input_adjoint = acot_wide + dot(table[...], unpack(3))
    atm_grad[...] = input_adjoint
    high, low = halves(input_adjoint)
    embed_high, embed_low = halves(embed[...])
    sa_send[...] = (
        dot_nt(embed_high, high) + dot_nt(embed_low, high) + dot_nt(embed_high, low)
    )
    band_to_groups(2, sa_send, sa_recv, start)

    def grad_store(row, begin, value):
        ocean_grad[row, pl.ds(begin, STEP), :] = value

    def grad_base(row, begin):
        return ocean_grad[row, pl.ds(begin, STEP), :]

    def given(row, begin):
        return ocot[row, pl.ds(begin, STEP), :].astype(F32)

    first_part(2, 1, True, given, grad_store)
    second_part(2, 1, True, grad_base, grad_store)

    outer_first(lambda row: backward(0, row, hid[0, row], ocean_grad[row], 3) and None)
    rims_start(3)

    near_wait(2, sa_recv)
    for row in range(rows):
        total = wa[0, row] * sa_recv[0]
        for slot in range(1, SLOTS):
            total = total + wa[slot, row] * sa_recv[slot]
        surf[row : row + 1, 0:lon] = total
    high, low = halves(surf[:, 0:lon])
    widened = (dot_nt(high, repeat[...]) + dot_nt(low, repeat[...])) * mask_value * (1.0 / ratio)
    surf[...] = widened

    first_part(3, 0, True, grad_base, grad_store)
    second_part(3, 0, True, grad_base, grad_store)

    def fold_row(row):
        masked = (mask_wide[row].astype(F32) * ocean_grad[row]).astype(BF16)
        fold[row] = dot_nt(flux_embed[...], masked)

    loop(rows, fold_row)
    for row in range(rows):
        high, low = halves(fold[row])
        fold[row, :, 0:lon] = dot(high, repeat[...]) + dot(low, repeat[...])

    def flux_part(slot):
        total = wo[slot, 0] * fold[0, :, 0:lon]
        for row in range(1, rows):
            total = total + wo[slot, row] * fold[row, :, 0:lon]
        fa_send[slot] = total

    loop(SLOTS, flux_part)
    group_to_bands(3, fa_send, fa_recv, start)

    read_rows = jnp.concatenate([read[...].astype(F32)] * rows, axis=1)
    block_read = jnp.where(inside, read_rows, 0.0).astype(BF16)
    high, low = halves(surf[...])
    share = dot_tn(high, block_read) + dot_tn(low, block_read)
    for row in range(rows):
        ocean_grad[row] = ocean_grad[row] + share[:, row * LANES : (row + 1) * LANES]

    near_wait(3, fa_recv)
    total = fa_recv[0]
    for slot in range(1, SLOTS // 2 * sections):
        total = total + fa_recv[slot]
    high, low = halves(total)
    rows_read = flux_read_t[...]
    atm_grad[...] = atm_grad[...] + dot_tn(high, rows_read) + dot_tn(low, rows_read)

    band_to_groups(0, flux_send, flux_recv, sent)
    group_to_bands(1, cp_send, cp_recv, sent)
    band_to_groups(2, sa_send, sa_recv, sent)
    group_to_bands(3, fa_send, fa_recv, sent)
    for index in range(xs.shape[0]):
        all_sent(index)
    for layer in range(win.shape[0]):
        rims_sent(layer)


def hand_over(*refs):
    count = (len(refs) - 2) // 3
    given, results, held = refs[:count], refs[count : 2 * count], refs[2 * count : 3 * count]
    arrived, left = refs[3 * count], refs[3 * count + 1]
    pieces = []
    for index in range(count):
        parts = given[index].shape[0] if len(given[index].shape) == 3 else 1
        for part in range(parts):
            at = (part,) if parts > 1 else (Ellipsis,)
            source, middle, place = (
                ref.at[at] for ref in (given[index], held[index], results[index])
            )
            first = pltpu.make_async_copy(source, middle, arrived.at[index, part])
            second = pltpu.make_async_copy(middle, place, left.at[index, part])
            first.start()
            pieces.append((first, second))
    for first, second in pieces:
        first.wait()
        second.start()
    for _, second in pieces:
        second.wait()


def per_device(
    atmosphere,
    ocean_state,
    land_mask,
    crossing_bands,
    ocean_regrid,
    atmosphere_regrid,
    surface_read,
    surface_embed,
    flux_read,
    flux_embed,
    legendre_forward,
    legendre_inverse,
    spectral_mix,
    conv_kernel,
    norm_gain,
    expand_weight,
    project_weight,
    atmosphere_cotangent,
    ocean_cotangent,
):
    axes = (lax.axis_size("sec"), lax.axis_size("tile"))
    devices = axes[0] * axes[1]
    lat_rows, lon, channels = atmosphere.shape
    rows, extent, ocean_channels = ocean_state.shape
    layers, side = conv_kernel.shape[0], conv_kernel.shape[1]
    fluxes = flux_read.shape[1]
    peers = crossing_bands.shape[1]
    modes, lat_count, _ = legendre_forward.shape
    cols = 2 * modes
    radius = side // 2
    assert lat_rows == 1 and lat_count == devices and devices == 2 * axes[1]
    assert layers == 2 and ocean_channels == LANES and extent % MARGIN == 0
    table = wave_table(lon, modes * devices)
    order = mode_order(lat_count, modes)
    operands = [
        atmosphere[0],
        ocean_state,
        land_mask,
        crossing_bands,
        ocean_regrid.reshape(peers, rows),
        atmosphere_regrid.reshape(peers, rows),
        surface_read[None, :],
        surface_embed.reshape(1, channels),
        flux_read.T,
        flux_embed,
        legendre_forward,
        legendre_inverse,
        spectral_mix,
        conv_kernel,
        norm_gain,
        expand_weight,
        project_weight,
        atmosphere_cotangent[0],
        ocean_cotangent,
        jnp.asarray(table),
        jnp.asarray(np.ascontiguousarray(table.T)),
        jnp.asarray(order),
        jnp.asarray(np.ascontiguousarray(order.T)),
    ]
    scalars = (3, 4, 5)
    near = SLOTS // 2 * axes[0]
    shape = (rows, extent, ocean_channels)
    outs = (
        jax.ShapeDtypeStruct((lon, channels), BF16),
        jax.ShapeDtypeStruct(shape, BF16),
        jax.ShapeDtypeStruct((lon, channels), F32),
        jax.ShapeDtypeStruct(shape, F32),
    )
    window = (rows + 2 * radius, extent + 2 * MARGIN, ocean_channels)
    block = cols * devices
    vmem = pltpu.VMEM
    results = pl.pallas_call(
        functools.partial(window_kernel, axes),
        out_shape=outs,
        in_specs=[
            pl.BlockSpec(memory_space=pltpu.SMEM if index in scalars else pltpu.VMEM)
            for index in range(len(operands))
        ],
        out_specs=tuple(pl.BlockSpec(memory_space=pltpu.VMEM) for _ in outs),
        scratch_shapes=[
            vmem((2 * layers,) + window, BF16),
            vmem(window, F32),
            vmem((layers,) + shape, F32),
            vmem((layers, side * side, STEP, ocean_channels), BF16),
            vmem(shape, BF16),
            vmem((extent, lon), BF16),
            vmem((rows, extent), F32),
            vmem((rows, lon, ocean_channels), BF16),
            vmem((rows, fluxes, extent), F32),
            pltpu.SMEM((SLOTS, rows), F32),
            pltpu.SMEM((SLOTS, rows), F32),
            vmem((fluxes, lon), F32),
            vmem((SLOTS, fluxes, lon), F32),
            vmem((SLOTS, 1, lon), F32),
            vmem((near, 1, lon), F32),
            vmem((1, lon), F32),
            vmem((SLOTS, 1, lon), F32),
            vmem((SLOTS, fluxes, lon), F32),
            vmem((near, fluxes, lon), F32),
            vmem((4, devices, cols, channels), BF16),
            vmem((4, devices, cols, channels), BF16),
            vmem((block, channels), F32),
            vmem((lon, channels), BF16),
            vmem((block, channels), BF16),
            vmem((block, channels), BF16),
            pltpu.SemaphoreType.DMA((2 * layers, 8)),
            pltpu.SemaphoreType.DMA((2 * layers, 8)),
            pltpu.SemaphoreType.DMA((2 * layers, 2 * radius)),
            pltpu.SemaphoreType.DMA((2 * layers, 2 * radius)),
            pltpu.SemaphoreType.DMA((4,)),
            pltpu.SemaphoreType.DMA((4,)),
            pltpu.SemaphoreType.DMA((4, SLOTS)),
            pltpu.SemaphoreType.DMA((4,)),
        ],
        compiler_params=pltpu.CompilerParams(
            collective_id=0, has_side_effects=True, vmem_limit_bytes=60 * 1024 * 1024
        ),
    )(*operands)
    results = pl.pallas_call(
        hand_over,
        out_shape=outs,
        in_specs=[pl.BlockSpec(memory_space=pl.ANY) for _ in outs],
        out_specs=tuple(pl.BlockSpec(memory_space=pl.ANY) for _ in outs),
        scratch_shapes=[vmem(out.shape, out.dtype) for out in outs]
        + [pltpu.SemaphoreType.DMA((len(outs), rows))] * 2,
    )(*results)
    atm_next, ocean_next, atm_grad, ocean_grad = results
    return (atm_next[None], ocean_next, atm_grad[None], ocean_grad)


def solution(mesh):
    return jax.shard_map(
        per_device,
        mesh=mesh,
        in_specs=(
            P(("sec", "tile"), None, None),
            P("tile", "sec", None),
            P("tile", "sec"),
            P("tile", None),
            P("tile", None, None, None),
            P("tile", None, None, None),
            P(),
            P(),
            P(),
            P(),
            P(("sec", "tile"), None, None),
            P(("sec", "tile"), None, None),
            P(),
            P(),
            P(),
            P(),
            P(),
            P(("sec", "tile"), None, None),
            P("tile", "sec", None),
        ),
        out_specs=(
            P(("sec", "tile"), None, None),
            P("tile", "sec", None),
            P(("sec", "tile"), None, None),
            P("tile", "sec", None),
        ),
        check_vma=False,
    )
```

```python
import functools

import jax
import jax.numpy as jnp
import numpy as np
from jax import lax
from jax.experimental import pallas as pl
from jax.experimental.pallas import tpu as pltpu
from jax.sharding import PartitionSpec as P

MESH = pl.DeviceIdType.MESH
F32 = jnp.float32
BF16 = jnp.bfloat16
GELU_SCALE = 0.7978845608028654
GELU_CUBIC = 0.044715
EPSILON = 1e-06
MARGIN = 16
SLOTS = 8
LANES = 128
STEP = 16


def wave_table(lon_count, mode_count):
    longitude = np.arange(lon_count)
    wavenumber = np.arange(mode_count)
    phase = (longitude[:, None] * wavenumber[None, :] % lon_count) * (2.0 * np.pi / lon_count)
    scaled = np.stack([np.cos(phase), -np.sin(phase)], axis=2) * np.sqrt(2.0 / lon_count)
    return scaled.reshape(lon_count, 2 * mode_count).astype(np.float32).astype(BF16)


def mode_order(lat_count, modes):
    source = np.arange(lat_count * modes * 2)
    lat, mode, part = source // (2 * modes), source % (2 * modes) // 2, source % 2
    matrix = np.zeros((source.size, source.size), np.float32)
    matrix[(part * modes + mode) * lat_count + lat, source] = 1.0
    return matrix.astype(BF16)


def dot(a, b):
    return lax.dot_general(a, b, (((1,), (0,)), ((), ())), preferred_element_type=F32)


def dot_nt(a, b):
    return lax.dot_general(a, b, (((1,), (1,)), ((), ())), preferred_element_type=F32)


def dot_tn(a, b):
    return lax.dot_general(a, b, (((0,), (0,)), ((), ())), preferred_element_type=F32)


def halves(x):
    high = x.astype(BF16)
    return high, (x - high.astype(F32)).astype(BF16)


def loop(count, body):
    def step(index, carry):
        body(index)
        return carry

    lax.fori_loop(0, count, step, jnp.int32(0))


def normalize(hidden):
    center = hidden - jnp.mean(hidden, axis=-1, keepdims=True)
    inverse_std = lax.rsqrt(jnp.mean(center * center, axis=-1, keepdims=True) + EPSILON)
    return center * inverse_std, inverse_std


def gelu_parts(before):
    square = before * before
    wave = jnp.tanh(before * (GELU_SCALE + (GELU_SCALE * GELU_CUBIC) * square))
    return square, wave


def gelu_value(before, wave):
    scaled = 0.5 * before
    return scaled + scaled * wave


def gelu_slope(before, square, wave):
    slope = (0.5 * GELU_SCALE + (1.5 * GELU_SCALE * GELU_CUBIC) * square) * before
    return (1.0 + wave) * (0.5 + slope * (1.0 - wave))


def staged_kernel(axes, late, total, *refs):
    ins, held, arrived = list(refs[:total]), refs[-1 - len(late) : -1], refs[-1]
    copies = []
    for place, index in enumerate(late):
        copies.append(pltpu.make_async_copy(ins[index], held[place], arrived.at[place]))
        copies[-1].start()
        ins[index] = held[place]

    def ready():
        for copy in copies:
            copy.wait()

    window_kernel(axes, ready, *ins, *refs[total : -1 - len(late)])


def window_kernel(
    axes, ready,
    atm, ocean, mask, bands, oreg, areg, read, embed, flux_read_t, flux_embed,
    leg_f, leg_i, smix, taps_in, gains, expand, project, acot, ocot,
    table, table_t, order, order_t,
    atm_next, ocean_next, atm_grad, ocean_grad,
    win, wide, hid, taps, mask_wide, repeat, surf, gall, fold,
    wo, wa, flux_send, flux_recv, cp_send, cp_recv, sa_send, sa_recv, fa_send, fa_recv,
    xs, xr, flat, mixed, spec_a, spec_b,
    halo_send, halo_recv, line_send, line_recv, x_send, x_recv, near_send, near_recv,
):
    sections, tiles = axes
    devices = sections * tiles
    sec = lax.axis_index("sec")
    tile = lax.axis_index("tile")
    me = sec * tiles + tile
    rows, extent, channels = ocean.shape
    lon = atm.shape[0]
    radius = (win.shape[1] - rows) // 2
    side = 2 * radius + 1
    part = lon // sections
    ratio = extent // part
    cols = xs.shape[2]
    right = MARGIN + extent

    def target(device):
        return {"sec": lax.div(device, tiles), "tile": lax.rem(device, tiles)}

    barrier = pltpu.get_barrier_semaphore()

    def greet(step):
        pl.semaphore_signal(
            barrier, inc=1, device_id=target(lax.rem(me + 1 + step, devices)), device_id_type=MESH
        )

    loop(devices - 1, greet)

    @pl.when(tile == 0)
    def _():
        win[:, 0:radius] = jnp.zeros((win.shape[0], radius) + win.shape[2:], BF16)

    @pl.when(tile == tiles - 1)
    def _():
        win[:, radius + rows :] = jnp.zeros((win.shape[0], radius) + win.shape[2:], BF16)

    x_index = lax.broadcasted_iota(jnp.int32, (extent, lon), 0)
    g_index = lax.broadcasted_iota(jnp.int32, (extent, lon), 1)
    offset = x_index - (g_index - sec * part) * ratio
    repeat[...] = jnp.where((offset >= 0) & (offset < ratio), 1.0, 0.0).astype(BF16)

    for row in range(rows):
        surf[row : row + 1, :] = dot_nt(read[...], ocean[row])
    mask_value = mask[...].astype(F32)
    high, low = halves(surf[...] * mask_value * (1.0 / ratio))
    surf[:, 0:lon] = dot(high, repeat[...]) + dot(low, repeat[...])

    flux_send[...] = dot_nt(flux_read_t[...], atm[...])

    def weights(slot):
        band = lax.rem(2 * tile - 2 + slot + devices, devices)
        for row in range(rows):
            to_ocean = jnp.float32(0.0)
            to_atm = jnp.float32(0.0)
            for peer in range(bands.shape[1]):
                same = jnp.where(bands[0, peer] == band, 1.0, 0.0)
                to_ocean = to_ocean + same * oreg[peer, row]
                to_atm = to_atm + same * areg[peer, row]
            wo[slot, row] = to_ocean
            wa[slot, row] = to_atm

    loop(SLOTS, weights)

    def coarse_part(slot):
        total = wa[slot, 0] * surf[0:1, 0:lon]
        for row in range(1, rows):
            total = total + wa[slot, row] * surf[row : row + 1, 0:lon]
        cp_send[slot] = total

    loop(SLOTS, coarse_part)

    pl.semaphore_wait(barrier, devices - 1)
    ready()

    def band_to_groups(index, source, slots, act):
        def one(step):
            turn, section = lax.div(step, sections), lax.rem(step, sections)
            group = lax.rem(lax.div(me, 2) + 1 - turn + tiles, tiles)
            slot = lax.rem(me, 2) + 2 * turn
            away = (section != sec) | (group != tile)

            def remote():
                return pltpu.make_async_remote_copy(
                    src_ref=source,
                    dst_ref=slots.at[slot],
                    send_sem=near_send.at[index, step],
                    recv_sem=near_recv.at[index],
                    device_id={"sec": section, "tile": group},
                    device_id_type=MESH,
                )

            @pl.when(away)
            def _():
                act(remote())

            if act is start:

                @pl.when(jnp.logical_not(away))
                def _():
                    pltpu.make_async_copy(source, slots.at[slot], near_recv.at[index]).start()

        loop(SLOTS // 2 * sections, one)

    def group_to_bands(index, parts, slots, act):
        def one(slot):
            band = lax.rem(2 * tile - 2 + slot + devices, devices)
            place = lax.div(slot, 2) * sections + sec

            def remote():
                return pltpu.make_async_remote_copy(
                    src_ref=parts.at[slot],
                    dst_ref=slots.at[place],
                    send_sem=near_send.at[index, slot],
                    recv_sem=near_recv.at[index],
                    device_id=target(band),
                    device_id_type=MESH,
                )

            @pl.when(band != me)
            def _():
                act(remote())

            if act is start:

                @pl.when(band == me)
                def _():
                    pltpu.make_async_copy(
                        parts.at[slot], slots.at[place], near_recv.at[index]
                    ).start()

        loop(SLOTS, one)

    def start(copy):
        copy.start()

    def sent(copy):
        copy.wait_send()

    def near_wait(index, slots):
        pltpu.make_async_copy(slots, slots, near_recv.at[index]).wait()

    def all_start(index):
        pltpu.make_async_copy(xs.at[index, me], xr.at[index, me], x_recv.at[index]).start()

        def one(step):
            peer = lax.rem(me + 1 + step, devices)
            pltpu.make_async_remote_copy(
                src_ref=xs.at[index, peer],
                dst_ref=xr.at[index, me],
                send_sem=x_send.at[index],
                recv_sem=x_recv.at[index],
                device_id=target(peer),
                device_id_type=MESH,
            ).start()

        loop(devices - 1, one)

    def all_wait(index):
        pltpu.make_async_copy(xr.at[index], xr.at[index], x_recv.at[index]).wait()

    def all_sent(index):
        others = xs.at[index, pl.ds(0, devices - 1)]
        pltpu.make_async_copy(others, others, x_send.at[index]).wait()

    def rim(layer, row_step, col_step):
        number = (row_step + 1) * 3 + col_step + 1
        number = number if number < 4 else number - 1
        source_rows = {-1: (radius, radius), 0: (radius, rows), 1: (rows, radius)}[row_step]
        place_rows = {-1: (radius + rows, radius), 0: (radius, rows), 1: (0, radius)}[row_step]
        inner = {-1: (MARGIN, MARGIN), 0: (MARGIN, extent), 1: (extent, MARGIN)}[col_step]
        outer = {-1: (right, MARGIN), 0: (MARGIN, extent), 1: (0, MARGIN)}[col_step]
        return pltpu.make_async_remote_copy(
            src_ref=win.at[layer, pl.ds(*source_rows), pl.ds(*inner)],
            dst_ref=win.at[layer, pl.ds(*place_rows), pl.ds(*outer)],
            send_sem=halo_send.at[layer, number],
            recv_sem=halo_recv.at[layer, number],
            device_id={
                "sec": lax.rem(sec + col_step + sections, sections),
                "tile": lax.rem(tile + row_step + tiles, tiles),
            },
            device_id_type=MESH,
        )

    def line_copy(layer, row_step, row, number):
        place = row + rows if row_step < 0 else row - rows
        return pltpu.make_async_remote_copy(
            src_ref=win.at[layer, row + radius, pl.ds(MARGIN, extent)],
            dst_ref=win.at[layer, place + radius, pl.ds(MARGIN, extent)],
            send_sem=line_send.at[layer, number],
            recv_sem=line_recv.at[layer, number],
            device_id={"sec": sec, "tile": lax.rem(tile + row_step + tiles, tiles)},
            device_id_type=MESH,
        )

    def line_start(layer, row):
        @pl.when((row < radius) & (tile != 0))
        def _():
            line_copy(layer, -1, row, row).start()

        @pl.when((row >= rows - radius) & (tile != tiles - 1))
        def _():
            line_copy(layer, 1, row, row - (rows - 2 * radius)).start()

    def outer_first(body):
        def one(index):
            half = lax.div(index, 2)
            body(jnp.where(lax.rem(index, 2) == 0, half, rows - 1 - half))

        loop(rows, one)

    def rims(layer, act, line_act, sending, row_steps):
        for row_step in row_steps:
            edge = {-1: 0, 0: None, 1: tiles - 1}[row_step if sending else -row_step]

            def each(row_step=row_step):
                if row_step != 0 and line_act is not None:
                    for step in range(radius):
                        row = step if row_step < 0 else rows - radius + step
                        number = row if row_step < 0 else row - (rows - 2 * radius)
                        line_act(line_copy(layer, row_step, row, number))
                for col_step in (-1, 1):
                    act(rim(layer, row_step, col_step))

            if edge is None:
                each()
            else:
                pl.when(tile != edge)(each)

    def rims_start(layer):
        rims(layer, lambda copy: copy.start(), None, True, (0, -1, 1))

    def rims_sent(layer):
        leave = lambda copy: copy.wait_send()
        rims(layer, leave, leave, True, (0, -1, 1))

    def rims_wait(layer, row_steps):
        arrive = lambda copy: copy.wait_recv()
        rims(layer, arrive, arrive, False, row_steps)

    def widen(layer, first, count):
        def one(index):
            wide[first + index] = win[layer, first + index].astype(F32)

        loop(count, one)

    def depthwise(kernel, flip, lines, base, store):
        def step(index):
            begin = pl.multiple_of(index * STEP, STEP)
            totals = [None] * rows
            for col in range(side):
                tap = [
                    taps[kernel, side * side - 1 - (u * side + col) if flip else u * side + col]
                    for u in range(side)
                ]
                if col % 2 == 0:
                    partial = [None] * rows
                for line in lines:
                    piece = wide[line, pl.ds(begin + (MARGIN - radius + col), STEP), :]
                    piece = piece.astype(BF16)
                    for u in range(side):
                        place = line - u
                        if 0 <= place < rows:
                            term = piece * tap[u]
                            old = partial[place]
                            partial[place] = term if old is None else old + term
                for row in range(rows):
                    if partial[row] is not None and (col % 2 == 1 or col == side - 1):
                        value = partial[row].astype(F32)
                        totals[row] = value if totals[row] is None else totals[row] + value
            for row in range(rows):
                if totals[row] is not None:
                    before = base(row, begin)
                    store(row, begin, totals[row] if before is None else before + totals[row])

        loop(extent // STEP, step)

    own_lines = range(radius, radius + rows)
    rim_lines = list(range(radius)) + list(range(radius + rows, rows + 2 * radius))

    def first_part(layer, kernel, flip, base, store):
        rims_wait(layer, (0,))
        widen(layer, radius, rows)
        depthwise(kernel, flip, own_lines, base, store)

    def second_part(layer, kernel, flip, base, store):
        rims_wait(layer, (-1, 1))
        widen(layer, 0, radius)
        widen(layer, radius + rows, radius)
        depthwise(kernel, flip, rim_lines, base, store)

    height = max(cols, 8)
    group = height // cols

    def unpack(index):
        def one(block):
            pieces = [
                xr[index, block * group + place].astype(F32) for place in range(group)
            ]
            flat[pl.ds(pl.multiple_of(block * height, height), height), :] = (
                pieces[0] if group == 1 else jnp.concatenate(pieces, axis=0)
            )

        loop(devices // group, one)
        return flat[...].astype(BF16)

    def pack(index, value):
        flat[...] = value

        def one(block):
            piece = flat[pl.ds(pl.multiple_of(block * height, height), height), :].astype(BF16)
            for place in range(group):
                xs[index, block * group + place] = piece[place * cols : (place + 1) * cols]

        loop(devices // group, one)
        all_start(index)

    def spectral(index, first, first_dot, second, second_dot, adjoint):
        modes, lat = first.shape[0], first.shape[1]
        half = modes * lat
        all_wait(index)
        spec_a[...] = dot(order[...], unpack(index)).astype(BF16)
        for block in range(2 * modes):
            piece = pl.ds(block * lat, lat)
            spec_b[piece] = first_dot(first[block % modes], spec_a[piece]).astype(BF16)
        real, imag = spec_b[0:half], spec_b[half : 2 * half]
        if adjoint:
            spec_a[0:half] = (dot_nt(real, smix[0]) + dot_nt(imag, smix[1])).astype(BF16)
            spec_a[half : 2 * half] = (dot_nt(imag, smix[0]) - dot_nt(real, smix[1])).astype(BF16)
        else:
            spec_a[0:half] = (dot(real, smix[0]) - dot(imag, smix[1])).astype(BF16)
            spec_a[half : 2 * half] = (dot(imag, smix[0]) + dot(real, smix[1])).astype(BF16)
        for block in range(2 * modes):
            piece = pl.ds(block * lat, lat)
            spec_b[piece] = second_dot(second[block % modes], spec_a[piece]).astype(BF16)
        pack(index + 1, dot(order_t[...], spec_b[...]))

    band_to_groups(0, flux_send, flux_recv, start)
    group_to_bands(1, cp_send, cp_recv, start)

    lane_row = lax.broadcasted_iota(jnp.int32, (rows, rows * LANES), 1)
    sub_row = lax.broadcasted_iota(jnp.int32, (rows, rows * LANES), 0)
    inside = (lane_row >= sub_row * LANES) & (lane_row < (sub_row + 1) * LANES)
    spread = jnp.where(inside, 1.0, 0.0).astype(BF16)
    column = dot_tn(mask_value.astype(BF16), spread)
    for row in range(rows):
        mask_wide[row] = column[:, row * LANES : (row + 1) * LANES].astype(BF16)

    for kernel in range(taps.shape[0]):
        for u in range(side):
            for v in range(side):
                tile_of = jnp.broadcast_to(taps_in[kernel, u, v : v + 1, :], (STEP, channels))
                taps[kernel, u * side + v] = tile_of.astype(BF16)

    near_wait(0, flux_recv)
    for row in range(rows):
        total = wo[0, row] * flux_recv[0]
        for slot in range(1, SLOTS):
            total = total + wo[slot, row] * flux_recv[slot]
        high, low = halves(total)
        embed_rows = flux_embed[...]
        gall[row] = (dot_tn(high, embed_rows) + dot_tn(low, embed_rows)).astype(BF16)

    def force(row):
        forcing = dot(repeat[...], gall[row])
        state = ocean[row].astype(F32) + mask_wide[row].astype(F32) * forcing
        win[0, row + radius, MARGIN:right, :] = state.astype(BF16)
        line_start(0, row)

    outer_first(force)
    rims_start(0)

    near_wait(1, cp_recv)
    total = cp_recv[0]
    for slot in range(1, SLOTS // 2 * sections):
        total = total + cp_recv[slot]
    high, low = halves(total)
    embed_high, embed_low = halves(embed[...])
    outer = dot_tn(
        jnp.concatenate([high, low, high], axis=0),
        jnp.concatenate([embed_high, embed_high, embed_low], axis=0),
    )
    mixed[...] = (atm[...].astype(F32) + outer).astype(BF16)
    pack(0, dot(table_t[...], mixed[...]))

    def forward_cells(layer, store):
        def cells(row):
            unit, _ = normalize(hid[layer, row])
            normed = (unit * gains[layer : layer + 1, :]).astype(BF16)
            before = dot(normed, expand[layer]).astype(BF16)
            _, wave = gelu_parts(before)
            active = gelu_value(before, wave)
            update = dot(active, project[layer])
            old = wide[row + radius, MARGIN:right, :]
            store(row, (old + mask_wide[row].astype(F32) * update).astype(BF16))

        outer_first(cells)

    def hidden_store(layer):
        def store(row, begin, value):
            hid[layer, row, pl.ds(begin, STEP), :] = value

        return store

    def hidden_base(layer):
        return lambda row, begin: hid[layer, row, pl.ds(begin, STEP), :]

    nothing = lambda row, begin: None

    first_part(0, 0, False, nothing, hidden_store(0))
    spectral(0, leg_f, dot, leg_i, dot, False)
    second_part(0, 0, False, hidden_base(0), hidden_store(0))

    def to_window(row, value):
        win[1, row + radius, MARGIN:right, :] = value
        line_start(1, row)

    forward_cells(0, to_window)
    rims_start(1)

    all_wait(1)
    response = dot(table[...], unpack(1))
    square, wave = gelu_parts(response)
    atm_next[...] = (mixed[...].astype(F32) + gelu_value(response, wave)).astype(BF16)
    slope = gelu_slope(response, square, wave)
    mixed[...] = (slope * acot[...].astype(F32)).astype(BF16)
    pack(2, dot(table_t[...], mixed[...]))

    first_part(1, 1, False, nothing, hidden_store(1))
    spectral(2, leg_i, dot_tn, leg_f, dot_tn, True)
    second_part(1, 1, False, hidden_base(1), hidden_store(1))

    def backward(layer, row, hidden, cotangent, window):
        gain = gains[layer : layer + 1, :]
        unit, inverse_std = normalize(hidden)
        normed = (unit * gain).astype(BF16)
        before = dot(normed, expand[layer]).astype(BF16)
        masked = (mask_wide[row].astype(F32) * cotangent).astype(BF16)
        active_adjoint = dot_nt(masked, project[layer]).astype(BF16)
        square, wave = gelu_parts(before)
        before_adjoint = gelu_slope(before, square, wave) * active_adjoint
        scaled = dot_nt(before_adjoint, expand[layer]) * gain
        adjoint = inverse_std * (
            scaled
            - jnp.mean(scaled, axis=-1, keepdims=True)
            - unit * jnp.mean(scaled * unit, axis=-1, keepdims=True)
        )
        win[window, row + radius, MARGIN:right, :] = adjoint.astype(BF16)
        line_start(window, row)
        return before, wave

    def turn(row):
        before, wave = backward(1, row, hid[1, row], ocot[row].astype(F32), 2)
        active = gelu_value(before, wave)
        update = dot(active, project[1])
        old = wide[row + radius, MARGIN:right, :]
        ocean_next[row] = (old + mask_wide[row].astype(F32) * update).astype(BF16)

    outer_first(turn)
    rims_start(2)

    all_wait(3)
    acot_wide = acot[...].astype(F32)
    input_adjoint = acot_wide + dot(table[...], unpack(3))
    atm_grad[...] = input_adjoint
    high, low = halves(input_adjoint)
    embed_high, embed_low = halves(embed[...])
    sa_send[...] = (
        dot_nt(embed_high, high) + dot_nt(embed_low, high) + dot_nt(embed_high, low)
    )
    band_to_groups(2, sa_send, sa_recv, start)

    def grad_store(row, begin, value):
        ocean_grad[row, pl.ds(begin, STEP), :] = value

    def grad_base(row, begin):
        return ocean_grad[row, pl.ds(begin, STEP), :]

    def given(row, begin):
        return ocot[row, pl.ds(begin, STEP), :].astype(F32)

    first_part(2, 1, True, given, grad_store)
    second_part(2, 1, True, grad_base, grad_store)

    outer_first(lambda row: backward(0, row, hid[0, row], ocean_grad[row], 3) and None)
    rims_start(3)

    near_wait(2, sa_recv)
    for row in range(rows):
        total = wa[0, row] * sa_recv[0]
        for slot in range(1, SLOTS):
            total = total + wa[slot, row] * sa_recv[slot]
        surf[row : row + 1, 0:lon] = total
    high, low = halves(surf[:, 0:lon])
    widened = (dot_nt(high, repeat[...]) + dot_nt(low, repeat[...])) * mask_value * (1.0 / ratio)
    surf[...] = widened

    first_part(3, 0, True, grad_base, grad_store)
    second_part(3, 0, True, grad_base, grad_store)

    def fold_row(row):
        masked = (mask_wide[row].astype(F32) * ocean_grad[row]).astype(BF16)
        fold[row] = dot_nt(flux_embed[...], masked)

    loop(rows, fold_row)
    for row in range(rows):
        high, low = halves(fold[row])
        fold[row, :, 0:lon] = dot(high, repeat[...]) + dot(low, repeat[...])

    def flux_part(slot):
        total = wo[slot, 0] * fold[0, :, 0:lon]
        for row in range(1, rows):
            total = total + wo[slot, row] * fold[row, :, 0:lon]
        fa_send[slot] = total

    loop(SLOTS, flux_part)
    group_to_bands(3, fa_send, fa_recv, start)

    read_rows = jnp.concatenate([read[...].astype(F32)] * rows, axis=1)
    block_read = jnp.where(inside, read_rows, 0.0).astype(BF16)
    high, low = halves(surf[...])
    share = dot_tn(high, block_read) + dot_tn(low, block_read)
    for row in range(rows):
        ocean_grad[row] = ocean_grad[row] + share[:, row * LANES : (row + 1) * LANES]

    near_wait(3, fa_recv)
    total = fa_recv[0]
    for slot in range(1, SLOTS // 2 * sections):
        total = total + fa_recv[slot]
    high, low = halves(total)
    rows_read = flux_read_t[...]
    atm_grad[...] = atm_grad[...] + dot_tn(high, rows_read) + dot_tn(low, rows_read)

    band_to_groups(0, flux_send, flux_recv, sent)
    group_to_bands(1, cp_send, cp_recv, sent)
    band_to_groups(2, sa_send, sa_recv, sent)
    group_to_bands(3, fa_send, fa_recv, sent)
    for index in range(xs.shape[0]):
        all_sent(index)
    for layer in range(win.shape[0]):
        rims_sent(layer)


def hand_over(*refs):
    count = (len(refs) - 2) // 3
    given, results, held = refs[:count], refs[count : 2 * count], refs[2 * count : 3 * count]
    arrived, left = refs[3 * count], refs[3 * count + 1]
    pieces = []
    for index in range(count):
        parts = given[index].shape[0] if len(given[index].shape) == 3 else 1
        for part in range(parts):
            at = (part,) if parts > 1 else (Ellipsis,)
            source, middle, place = (
                ref.at[at] for ref in (given[index], held[index], results[index])
            )
            first = pltpu.make_async_copy(source, middle, arrived.at[index, part])
            second = pltpu.make_async_copy(middle, place, left.at[index, part])
            first.start()
            pieces.append((first, second))
    for first, second in pieces:
        first.wait()
        second.start()
    for _, second in pieces:
        second.wait()


def per_device(
    atmosphere,
    ocean_state,
    land_mask,
    crossing_bands,
    ocean_regrid,
    atmosphere_regrid,
    surface_read,
    surface_embed,
    flux_read,
    flux_embed,
    legendre_forward,
    legendre_inverse,
    spectral_mix,
    conv_kernel,
    norm_gain,
    expand_weight,
    project_weight,
    atmosphere_cotangent,
    ocean_cotangent,
):
    axes = (lax.axis_size("sec"), lax.axis_size("tile"))
    devices = axes[0] * axes[1]
    lat_rows, lon, channels = atmosphere.shape
    rows, extent, ocean_channels = ocean_state.shape
    layers, side = conv_kernel.shape[0], conv_kernel.shape[1]
    fluxes = flux_read.shape[1]
    peers = crossing_bands.shape[1]
    modes, lat_count, _ = legendre_forward.shape
    cols = 2 * modes
    radius = side // 2
    assert lat_rows == 1 and lat_count == devices and devices == 2 * axes[1]
    assert layers == 2 and ocean_channels == LANES and extent % MARGIN == 0
    table = wave_table(lon, modes * devices)
    order = mode_order(lat_count, modes)
    operands = [
        atmosphere[0],
        ocean_state,
        land_mask,
        crossing_bands,
        ocean_regrid.reshape(peers, rows),
        atmosphere_regrid.reshape(peers, rows),
        surface_read[None, :],
        surface_embed.reshape(1, channels),
        flux_read.T,
        flux_embed,
        legendre_forward,
        legendre_inverse,
        spectral_mix,
        conv_kernel,
        norm_gain,
        expand_weight,
        project_weight,
        atmosphere_cotangent[0],
        ocean_cotangent,
        jnp.asarray(table),
        jnp.asarray(np.ascontiguousarray(table.T)),
        jnp.asarray(order),
        jnp.asarray(np.ascontiguousarray(order.T)),
    ]
    scalars = (3, 4, 5)
    late = (10, 11, 12, 15, 16, 17, 18, 19, 20, 21, 22)
    near = SLOTS // 2 * axes[0]
    shape = (rows, extent, ocean_channels)
    outs = (
        jax.ShapeDtypeStruct((lon, channels), BF16),
        jax.ShapeDtypeStruct(shape, BF16),
        jax.ShapeDtypeStruct((lon, channels), F32),
        jax.ShapeDtypeStruct(shape, F32),
    )
    window = (rows + 2 * radius, extent + 2 * MARGIN, ocean_channels)
    block = cols * devices
    vmem = pltpu.VMEM
    results = pl.pallas_call(
        functools.partial(staged_kernel, axes, late, len(operands)),
        out_shape=outs,
        in_specs=[
            pl.BlockSpec(
                memory_space=pltpu.SMEM
                if index in scalars
                else pl.ANY if index in late else pltpu.VMEM
            )
            for index in range(len(operands))
        ],
        out_specs=tuple(pl.BlockSpec(memory_space=pltpu.VMEM) for _ in outs),
        scratch_shapes=[
            vmem((2 * layers,) + window, BF16),
            vmem(window, F32),
            vmem((layers,) + shape, F32),
            vmem((layers, side * side, STEP, ocean_channels), BF16),
            vmem(shape, BF16),
            vmem((extent, lon), BF16),
            vmem((rows, extent), F32),
            vmem((rows, lon, ocean_channels), BF16),
            vmem((rows, fluxes, extent), F32),
            pltpu.SMEM((SLOTS, rows), F32),
            pltpu.SMEM((SLOTS, rows), F32),
            vmem((fluxes, lon), F32),
            vmem((SLOTS, fluxes, lon), F32),
            vmem((SLOTS, 1, lon), F32),
            vmem((near, 1, lon), F32),
            vmem((1, lon), F32),
            vmem((SLOTS, 1, lon), F32),
            vmem((SLOTS, fluxes, lon), F32),
            vmem((near, fluxes, lon), F32),
            vmem((4, devices, cols, channels), BF16),
            vmem((4, devices, cols, channels), BF16),
            vmem((block, channels), F32),
            vmem((lon, channels), BF16),
            vmem((block, channels), BF16),
            vmem((block, channels), BF16),
            pltpu.SemaphoreType.DMA((2 * layers, 8)),
            pltpu.SemaphoreType.DMA((2 * layers, 8)),
            pltpu.SemaphoreType.DMA((2 * layers, 2 * radius)),
            pltpu.SemaphoreType.DMA((2 * layers, 2 * radius)),
            pltpu.SemaphoreType.DMA((4,)),
            pltpu.SemaphoreType.DMA((4,)),
            pltpu.SemaphoreType.DMA((4, SLOTS)),
            pltpu.SemaphoreType.DMA((4,)),
        ]
        + [vmem(operands[index].shape, operands[index].dtype) for index in late]
        + [pltpu.SemaphoreType.DMA((len(late),))],
        compiler_params=pltpu.CompilerParams(
            collective_id=0, has_side_effects=True, vmem_limit_bytes=60 * 1024 * 1024
        ),
    )(*operands)
    results = pl.pallas_call(
        hand_over,
        out_shape=outs,
        in_specs=[pl.BlockSpec(memory_space=pl.ANY) for _ in outs],
        out_specs=tuple(pl.BlockSpec(memory_space=pl.ANY) for _ in outs),
        scratch_shapes=[vmem(out.shape, out.dtype) for out in outs]
        + [pltpu.SemaphoreType.DMA((len(outs), rows))] * 2,
    )(*results)
    atm_next, ocean_next, atm_grad, ocean_grad = results
    return (atm_next[None], ocean_next, atm_grad[None], ocean_grad)


def solution(mesh):
    return jax.shard_map(
        per_device,
        mesh=mesh,
        in_specs=(
            P(("sec", "tile"), None, None),
            P("tile", "sec", None),
            P("tile", "sec"),
            P("tile", None),
            P("tile", None, None, None),
            P("tile", None, None, None),
            P(),
            P(),
            P(),
            P(),
            P(("sec", "tile"), None, None),
            P(("sec", "tile"), None, None),
            P(),
            P(),
            P(),
            P(),
            P(),
            P(("sec", "tile"), None, None),
            P("tile", "sec", None),
        ),
        out_specs=(
            P(("sec", "tile"), None, None),
            P("tile", "sec", None),
            P(("sec", "tile"), None, None),
            P("tile", "sec", None),
        ),
        check_vma=False,
    )
```
